32 devices in a mesh: stream: 8 (over y, x, core), leaf: 4 (over z).
Axes of the slice: x: 2, y: 2, z: 4, core: 2. Of those that a mesh axis runs over, the one named last changes fastest.
Arguments:
- points_rhs: bfloat16 [2048, 32, 128], P(('stream', 'leaf')), may hold values from -6 to 6
- leaf_basis: bfloat16 [2048, 64, 128], P(('stream', 'leaf')), may hold values from -0.5 to 0.5
- transfer: bfloat16 [1024, 64, 128], P(('stream', 'leaf')), may hold values from -0.5 to 0.5
- leaf_coupling: bfloat16 [2048, 64, 256], P(('stream', 'leaf')), may hold values from -0.375 to 0.375
- parent_coupling: bfloat16 [1024, 64, 512], P(('stream', 'leaf')), may hold values from -0.25 to 0.25
- near_blocks: bfloat16 [2048, 3, 128, 128], P(('stream', 'leaf')), may hold values from -0.3125 to 0.3125
- near_offsets: int32 [2048, 3], P(('stream', 'leaf')), may hold values from -2 to 2, as said below
- coupling_offsets: int32 [2048, 4], P(('stream', 'leaf')), may hold values from -5 to 5, as said below
- parent_owner: int32 [1024, 8], P(('stream', 'leaf')), may hold values from 0 to 31, all different within a row; in each aligned block of 32 rows (0 to 31, 32 to 63, ...) at most 16 rows name the same one
- parent_local: int32 [1024, 8], P(('stream', 'leaf')), may hold values from 0 to 31
Outputs:
- product: bfloat16 [2048, 32, 128], P(('stream', 'leaf'))
The draws below stay inside these ranges and needn't reach their ends.
Inputs may be any that keep to these rules, and one draw needn't show every extreme that they name: `near_offsets`: each row holds 3 different offsets; the first is 0. `coupling_offsets`: each row holds 4 different nonzero offsets, none of which stands in the same row of near_offsets. `parent_owner`: each row names 8 different blocks; the rows of one device name no block more than 16 times, and in every draw some block is named exactly 16 times by the rows of some device.
All inputs are finite; a program needn't handle non-finite values.
Results may differ from the reference program's by a relative error of at most 0.0053.
Values may be sent and summed in bfloat16 or wider, within the bound.
No kernel may reach another device: no remote copies, remote signals or barrier semaphores. Data moves between devices by JAX's collectives and lax.ppermute only.
A program may use at most 128 MiB of HBM per device.

```python
import math
import jax
import jax.numpy as jnp
import numpy as np
from jax import lax

R = 64
NRHS = 32
LS = 128
KN = 3
KC = 4
KP = 8
LEAF_DEV = 64
PAR_DEV = 32
NLEAF = 2048
NPAR = 1024
CAP = 16
DEVICES = 32


def leaf_lists(key):
    key_near = jax.random.fold_in(key, 11)
    key_far = jax.random.fold_in(key, 23)
    near_pool = jnp.array([-2, -1, 1, 2], jnp.int32)
    far_pool = jnp.array([-5, -4, -3, 3, 4, 5], jnp.int32)
    near_scores = jax.random.randint(key_near, (NLEAF, 4), 0, 1 << 20, dtype=jnp.int32) * 16 + jnp.arange(4, dtype=jnp.int32)
    near_order = jnp.argsort(near_scores, axis=1, stable=True)
    chosen = near_pool[near_order]
    near_rows = jnp.concatenate([jnp.zeros((NLEAF, 1), jnp.int32), chosen[:, :KN - 1]], axis=1)
    remaining = jnp.concatenate([chosen[:, KN - 1:], jnp.broadcast_to(far_pool, (NLEAF, 6))], axis=1)
    pool_size = 11 - KN
    far_scores = jax.random.randint(key_far, (NLEAF, pool_size), 0, 1 << 20, dtype=jnp.int32) * 16 + jnp.arange(pool_size, dtype=jnp.int32)
    far_order = jnp.argsort(far_scores, axis=1, stable=True)
    far_rows = jnp.take_along_axis(remaining, far_order, axis=1)[:, :KC]
    return (near_rows, far_rows)


def draw_near_offsets(key, part):
    return leaf_lists(key)[0]


def draw_coupling_offsets(key, part):
    return leaf_lists(key)[1]


def set_ends(entries, key, low, top_value):
    dims = entries.shape
    index_at = [jax.random.randint(jax.random.fold_in(key, axis), (), 0, dims[axis]) for axis in range(len(dims))]
    entries = entries.at[tuple(index_at)].set(low)
    longest = dims.index(max(dims))
    index_at[longest] = (index_at[longest] + 1) % dims[longest]
    return entries.at[tuple(index_at)].set(top_value)


def steps_of(stream_key, shape, pieces, smallest, largest):
    def one(dim, shards_of):
        draws = jax.random.uniform(jax.random.fold_in(jax.random.fold_in(stream_key, 6), dim), (shards_of,), jnp.float32, smallest / len(pieces), largest / len(pieces))
        return jnp.repeat(jnp.exp(draws), shape[dim] // shards_of).reshape((-1,) + (1,) * (len(shape) - dim - 1))

    level = one(*pieces[0])
    for cut in pieces[1:]:
        level = level * one(*cut)
    return level


def deal_out(own_key, own, number, rows, amount, top, bound, skew):
    sequence = jax.random.permutation(own_key, amount)
    crowded, usual = portions_of(amount, rows * top, bound, skew, True), portions_of(amount, rows * top, bound, skew, False)
    places = jnp.arange(amount)

    def named(sizes, turn):
        used = int((sizes > 0).sum())
        fixed = max(1, used // 4)
        moved = fixed + (places - fixed + turn * (used - fixed)) % max(1, amount - fixed)
        return jnp.zeros((amount,), jnp.int32).at[sequence[jnp.where(places < fixed, places, moved)]].set(jnp.asarray(sizes, jnp.int32))

    sizes = jnp.where(number % 4 == 0, named(crowded, number // 4), named(usual, number - number // 4 - 1))
    mixed = jax.random.permutation(jax.random.fold_in(own, 3), amount)
    source_of, taker = mixed[0:amount // 2 * 2:2], mixed[1:amount // 2 * 2:2]
    room = jnp.minimum(sizes[source_of] - 1, bound - sizes[taker]) // 2
    room = jnp.where((source_of == sequence[0]) | (taker == sequence[0]) | (sizes[taker] == 0), 0, jnp.maximum(room, 0))
    moved = jax.random.randint(jax.random.fold_in(own, 4), (amount // 2,), 0, 1 << 20) % (room + 1)
    sizes = sizes.at[source_of].add(-moved).at[taker].add(moved)
    labels = jnp.searchsorted(jnp.cumsum(sizes), jnp.arange(rows * top), side="right").astype(jnp.int32)
    listing = labels.reshape(top, rows).T
    listing = listing[jax.random.permutation(jax.random.fold_in(own, 1), rows)]
    turn = jax.random.randint(jax.random.fold_in(own, 2), (rows, 1), 0, top)
    return jnp.take_along_axis(listing, (jnp.arange(top)[None, :] + turn) % top, axis=1)


def portions_of(amount, total, most, lean, full):
    weights = [(1 << 20) // math.isqrt(rank ** lean) + 1 for rank in range(1, amount + 1)]
    largest = most if full else min(most, max(-(-total // amount), total * weights[0] // sum(weights)))
    least = 1 if total - largest >= amount - 1 else 0
    holding, rest = [largest] + [least] * (amount - 1), total - largest - least * (amount - 1)
    while rest > 0:
        movable = [i for i in range(1, amount) if holding[i] < largest] or [i for i in range(1, amount) if holding[i] < most]
        pool, left = sum([weights[i] for i in movable]), rest
        for i in movable:
            addition = min(most - holding[i], max(1, left * weights[i] // pool), rest)
            holding[i] = holding[i] + addition
            rest = rest - addition
    return np.array(holding)


def scatter_about(rng, shape, spread, reach, shards=(), kind=jnp.bfloat16):
    drawn = spread * jax.random.normal(rng, shape, jnp.float32)
    if shards:
        drawn = drawn * steps_of(rng, shape, shards, -0.22, 0.18)
    return jnp.clip(drawn, -reach, reach).astype(kind)


def setup_inputs(seed: int = 0) -> dict:
    key_list = jax.random.split(jax.random.key(seed), 11)
    points_rhs = scatter_about(key_list[0], (NLEAF, NRHS, LS), 1.0, 6.0, ((0, 32),))
    leaf_basis = scatter_about(key_list[1], (NLEAF, R, LS), LS ** -0.5, 0.5, ((0, 32),))
    transfer = scatter_about(key_list[2], (NPAR, R, 2 * R), (2 * R) ** -0.5, 0.5, ((0, 32),))
    leaf_coupling = scatter_about(key_list[3], (NLEAF, R, KC * R), (KC * R) ** -0.5, 0.375, ((0, 32),))
    parent_coupling = scatter_about(key_list[4], (NPAR, R, KP * R), (KP * R) ** -0.5, 0.25, ((0, 32),))
    near_blocks = scatter_about(key_list[5], (NLEAF, KN, LS, LS), (KN * LS) ** -0.5, 0.3125, ((0, 32),))
    near_offsets = draw_near_offsets(jax.random.fold_in(key_list[10], 71), 0)
    coupling_offsets = draw_coupling_offsets(jax.random.fold_in(key_list[10], 71), 0)
    parent_owner_keys = jax.random.split(jax.random.fold_in(key_list[8], 1), NPAR // PAR_DEV)
    parent_owner_turns = jax.random.permutation(jax.random.fold_in(key_list[8], 3), NPAR // PAR_DEV)
    parent_owner = jax.vmap(lambda own, number: deal_out(jax.random.fold_in(key_list[8], 2), own, number, PAR_DEV, DEVICES, KP, CAP, 1))(parent_owner_keys, parent_owner_turns).reshape((NPAR, KP))
    parent_local = set_ends(jax.random.randint(key_list[9], (NPAR, KP), 0, PAR_DEV), jax.random.fold_in(key_list[9], 1), 0, PAR_DEV - 1).astype(jnp.int32)
    return {"points_rhs": points_rhs, "leaf_basis": leaf_basis, "transfer": transfer, "leaf_coupling": leaf_coupling, "parent_coupling": parent_coupling, "near_blocks": near_blocks, "near_offsets": near_offsets, "coupling_offsets": coupling_offsets, "parent_owner": parent_owner, "parent_local": parent_local}


def shifted_rows(padded, offsets, reach_leaves):
    row_count = offsets.shape[0]
    row_base = jnp.arange(row_count, dtype=jnp.int32)[:, None] + reach_leaves
    return padded[(row_base + offsets).astype(jnp.int32)]


def near_block(paired):
    return jnp.einsum('cknj,ckqj->cnq', paired[0].astype(jnp.float32), paired[1].astype(jnp.float32))


def reference(points_rhs, leaf_basis, transfer, leaf_coupling, parent_coupling, near_blocks, near_offsets, coupling_offsets, parent_owner, parent_local):
    leaf_coeffs = jnp.einsum('cnp,crp->cnr', points_rhs.astype(jnp.float32), leaf_basis.astype(jnp.float32)).astype(jnp.bfloat16)
    paired = leaf_coeffs.reshape(NPAR, 2, NRHS, R).transpose(0, 2, 1, 3).reshape(NPAR, NRHS, 2 * R)
    parent_coeffs = jnp.einsum('pnk,prk->pnr', paired.astype(jnp.float32), transfer.astype(jnp.float32)).astype(jnp.bfloat16)
    coeff_padded = jnp.pad(leaf_coeffs, ((5, 5), (0, 0), (0, 0)))
    sources = shifted_rows(coeff_padded, coupling_offsets, 5)
    coupling_panel = leaf_coupling.reshape(NLEAF, R, KC, R)
    leaf_field = jnp.einsum('cknj,crkj->cnr', sources.astype(jnp.float32), coupling_panel.astype(jnp.float32))
    source_rows = (parent_owner * PAR_DEV + parent_local).astype(jnp.int32)
    remote = parent_coeffs[source_rows]
    parent_panel = parent_coupling.reshape(NPAR, R, KP, R)
    parent_field = jnp.einsum('pknj,prkj->pnr', remote.astype(jnp.float32), parent_panel.astype(jnp.float32))
    parent_half = lax.optimization_barrier(parent_field.astype(jnp.bfloat16))
    downward = jnp.einsum('pnr,prk->pnk', parent_half.astype(jnp.float32), transfer.astype(jnp.float32))
    downward = downward.reshape(NPAR, NRHS, 2, R).transpose(0, 2, 1, 3).reshape(NLEAF, NRHS, R)
    leaf_total = (leaf_field + downward).astype(jnp.bfloat16)
    far_terms = jnp.einsum('cnr,crp->cnp', leaf_total.astype(jnp.float32), leaf_basis.astype(jnp.float32))
    point_padded = jnp.pad(points_rhs, ((2, 2), (0, 0), (0, 0)))
    near_rows = shifted_rows(point_padded, near_offsets, 2).reshape(DEVICES, LEAF_DEV, KN, NRHS, LS)
    block_rows = near_blocks.reshape(DEVICES, LEAF_DEV, KN, LS, LS)
    near_terms = lax.map(near_block, (near_rows, block_rows)).reshape(NLEAF, NRHS, LS)
    return (far_terms + near_terms).astype(jnp.bfloat16)
```

```python
import functools

import jax
import jax.numpy as jnp
from jax import lax
from jax.experimental import pallas as pl
from jax.experimental.pallas import tpu as pltpu
from jax.sharding import PartitionSpec as P

AXES = ("stream", "leaf")
FAR = 5
NEAR = 2
F32 = jnp.float32
BF16 = jnp.bfloat16


def dot_t(a, b):
    return lax.dot_general(a, b, (((1,), (1,)), ((), ())), preferred_element_type=F32)


def dot_n(a, b):
    return lax.dot_general(a, b, (((1,), (0,)), ((), ())), preferred_element_type=F32)


def left_half(rows, lanes):
    return lax.broadcasted_iota(jnp.int32, (rows, lanes), 1) < lanes // 2


def swap_halves(tile):
    half = tile.shape[1] // 2
    return jnp.concatenate([tile[:, half:], tile[:, :half]], axis=1)


def dense(doubled, mask):
    half = doubled.shape[0] // 2
    return jnp.where(mask, doubled[:half], doubled[half:]).astype(BF16)


def upward_kernel(par_ref, pts_ref, basis_ref, trans_ref, coeff_ref, pay_ref, side_ref, *, steps, parents):
    step = pl.program_id(0)
    pairs = trans_ref.shape[0]
    n = pts_ref.shape[1]
    wide = left_half(n, 128)
    mask = left_half(n // 2, 128)
    for p in range(pairs):
        halves = []
        for j in (0, 1):
            b = basis_ref[2 * p + j]
            c = dot_t(pts_ref[2 * p + j], jnp.concatenate([b, b], axis=0))
            coeff_ref[2 * p + j] = dense(c, mask)
            halves.append(c)
        paired = jnp.where(wide, halves[0], halves[1]).astype(BF16)
        t = trans_ref[p]
        up = dot_t(paired, jnp.concatenate([t, t], axis=0))
        pay_ref[step * pairs + p] = dense(up, mask)

    def edge(ref, at, first):
        leaves = pts_ref.shape[0]
        lo = 0 if first else leaves - FAR
        for q in range(FAR):
            ref[at + q] = coeff_ref[lo + q]
        lo = 0 if first else leaves - NEAR
        for q in range(NEAR):
            x = pts_ref[lo + q]
            ref[at + FAR + 2 * q] = x[: n // 2]
            ref[at + FAR + 2 * q + 1] = x[n // 2 :]

    odd = par_ref[0] == 1

    @pl.when(step == 0)
    def _():
        @pl.when(odd)
        def _():
            edge(pay_ref, parents, True)

        @pl.when(jnp.logical_not(odd))
        def _():
            edge(side_ref, 0, True)

    @pl.when(step == steps - 1)
    def _():
        @pl.when(odd)
        def _():
            edge(side_ref, 0, False)

        @pl.when(jnp.logical_not(odd))
        def _():
            edge(pay_ref, parents, False)


def upward(par, points, basis, transfer):
    leaves, n, size = points.shape
    parents, rank, _ = transfer.shape
    steps = 4
    lc, pc = leaves // steps, parents // steps
    halo = FAR + 2 * NEAR
    tile = (n // 2, 2 * rank)
    return pl.pallas_call(
        functools.partial(upward_kernel, steps=steps, parents=parents),
        out_shape=(
            jax.ShapeDtypeStruct((leaves,) + tile, BF16),
            jax.ShapeDtypeStruct((parents + halo,) + tile, BF16),
            jax.ShapeDtypeStruct((halo,) + tile, BF16),
        ),
        grid_spec=pltpu.PrefetchScalarGridSpec(
            num_scalar_prefetch=1,
            grid=(steps,),
            in_specs=[
                pl.BlockSpec((lc, n, size), lambda i, s: (i, 0, 0)),
                pl.BlockSpec((lc, rank, size), lambda i, s: (i, 0, 0)),
                pl.BlockSpec((pc, rank, 2 * rank), lambda i, s: (i, 0, 0)),
            ],
            out_specs=[
                pl.BlockSpec((lc,) + tile, lambda i, s: (i, 0, 0)),
                pl.BlockSpec((parents + halo,) + tile, lambda i, s: (0, 0, 0)),
                pl.BlockSpec((halo,) + tile, lambda i, s: (0, 0, 0)),
            ],
        ),
        name="upward",
    )(par, points, basis, transfer)


def local_kernel(
    par_ref, noff_ref, coff_ref, pts_ref, coeff_ref, pay_ref, side_ref, near_ref, coup_ref,
    near_out, field_out, pts_pad, coeff_pad, *, parents
):
    step = pl.program_id(0)
    leaves = pts_ref.shape[0]
    n = pts_ref.shape[1]
    chunk = near_ref.shape[0]
    mask = left_half(n // 2, 128)
    wide = left_half(n, 128)

    @pl.when(step == 0)
    def _():
        pts_pad[NEAR : NEAR + leaves] = pts_ref[...]
        coeff_pad[FAR : FAR + leaves] = coeff_ref[...]

        def put(ref, at, low):
            co = 0 if low else leaves + FAR
            po = 0 if low else leaves + NEAR
            for q in range(FAR):
                coeff_pad[co + q] = ref[at + q]
            for q in range(NEAR):
                pts_pad[po + q, : n // 2] = ref[at + FAR + 2 * q]
                pts_pad[po + q, n // 2 :] = ref[at + FAR + 2 * q + 1]

        odd = par_ref[0] == 1

        @pl.when(odd)
        def _():
            put(pay_ref, parents, True)
            put(side_ref, 0, False)

        @pl.when(jnp.logical_not(odd))
        def _():
            put(side_ref, 0, True)
            put(pay_ref, parents, False)

    slots = near_ref.shape[1]
    far_slots = coff_ref.shape[1]
    fields = []
    for j in range(chunk):
        c = step * chunk + j
        xs = [pts_pad[c + NEAR + noff_ref[c, k]] for k in range(slots)]
        ws = [near_ref[j, k] for k in range(slots)]
        near_out[j] = dot_t(jnp.concatenate(xs, axis=1), jnp.concatenate(ws, axis=1))
        tops, bots = [], []
        for k in range(0, far_slots, 2):
            a = coeff_pad[c + FAR + coff_ref[c, k]]
            b = coeff_pad[c + FAR + coff_ref[c, k + 1]]
            tops.append(jnp.where(mask, a, swap_halves(b)))
            bots.append(jnp.where(mask, swap_halves(a), b))
        lhs = jnp.concatenate([jnp.concatenate(tops, axis=1), jnp.concatenate(bots, axis=1)], axis=0)
        w = coup_ref[j]
        fields.append(dot_t(lhs, jnp.concatenate([w, w], axis=0)))
    for j in range(0, chunk, 2):
        field_out[j // 2] = jnp.where(wide, fields[j], fields[j + 1])


def local_terms(par, near_offsets, coupling_offsets, points, coeffs, payload, side, near_blocks, leaf_coupling):
    leaves, n, size = points.shape
    rank = leaf_coupling.shape[1]
    slots = near_blocks.shape[1]
    chunk = 8
    halo = side.shape[0]
    parents = payload.shape[0] - halo
    tile = side.shape[1:]
    whole = lambda i, *s: (0, 0, 0)
    return pl.pallas_call(
        functools.partial(local_kernel, parents=parents),
        out_shape=(
            jax.ShapeDtypeStruct((leaves, n, size), F32),
            jax.ShapeDtypeStruct((leaves // 2, n, 2 * rank), F32),
        ),
        grid_spec=pltpu.PrefetchScalarGridSpec(
            num_scalar_prefetch=3,
            grid=(leaves // chunk,),
            in_specs=[
                pl.BlockSpec(points.shape, whole),
                pl.BlockSpec(coeffs.shape, whole),
                pl.BlockSpec(payload.shape, whole),
                pl.BlockSpec(side.shape, whole),
                pl.BlockSpec((chunk, slots, size, size), lambda i, *s: (i, 0, 0, 0)),
                pl.BlockSpec((chunk,) + leaf_coupling.shape[1:], lambda i, *s: (i, 0, 0)),
            ],
            out_specs=[
                pl.BlockSpec((chunk, n, size), lambda i, *s: (i, 0, 0)),
                pl.BlockSpec((chunk // 2, n, 2 * rank), lambda i, *s: (i, 0, 0)),
            ],
            scratch_shapes=[
                pltpu.VMEM((leaves + 2 * NEAR, n, size), BF16),
                pltpu.VMEM((leaves + 2 * FAR,) + tile, BF16),
            ],
        ),
        name="local_terms",
    )(par, near_offsets, coupling_offsets, points, coeffs, payload, side, near_blocks, leaf_coupling)


def downward_kernel(me_ref, owner_ref, local_ref, *refs, starts, parents):
    count = len(starts)
    blocks = refs[:count]
    coup_ref, trans_ref, basis_ref, near_ref, field_ref, out_ref, table, sems = refs[count:]
    step = pl.program_id(0)
    pairs = trans_ref.shape[0]
    n = near_ref.shape[1]
    slots = owner_ref.shape[1]
    mask = left_half(n // 2, 128)

    @pl.when(step == 0)
    def _():
        copies = []
        for i, (ref, at) in enumerate(zip(blocks, starts)):
            rows = ref.shape[0] // parents * parents
            copies.append(
                pltpu.make_async_copy(ref.at[pl.ds(0, rows)], table.at[pl.ds(at, rows)], sems.at[i])
            )
        for c in copies:
            c.start()
        for c in copies:
            c.wait()

    zero = jnp.zeros(basis_ref.shape[1:], BF16)
    me = me_ref[0]
    for p in range(pairs):
        row = step * pairs + p
        tops, bots = [], []
        for k in range(0, slots, 2):
            a = table[(owner_ref[row, k] ^ me) * parents + local_ref[row, k]]
            b = table[(owner_ref[row, k + 1] ^ me) * parents + local_ref[row, k + 1]]
            tops.append(jnp.where(mask, a, swap_halves(b)))
            bots.append(jnp.where(mask, swap_halves(a), b))
        lhs = jnp.concatenate([jnp.concatenate(tops, axis=1), jnp.concatenate(bots, axis=1)], axis=0)
        half = dot_t(lhs, coup_ref[p]).astype(BF16)
        down = dot_n(half, trans_ref[p])
        total = (field_ref[p] + down).astype(BF16)
        spread = jnp.concatenate(
            [
                jnp.concatenate([basis_ref[2 * p], zero], axis=1),
                jnp.concatenate([zero, basis_ref[2 * p + 1]], axis=1),
            ],
            axis=0,
        )
        far = dot_n(total, spread)
        size = near_ref.shape[2]
        out_ref[2 * p] = (far[:, :size] + near_ref[2 * p]).astype(BF16)
        out_ref[2 * p + 1] = (far[:, size:] + near_ref[2 * p + 1]).astype(BF16)


def downward(me, owner, local, blocks, starts, coupling, transfer, basis, near, field, devices):
    leaves, n, size = near.shape
    parents, rank, _ = transfer.shape
    steps = 4
    lc, pc = leaves // steps, parents // steps
    at3 = lambda i, *s: (i, 0, 0)
    return pl.pallas_call(
        functools.partial(downward_kernel, starts=tuple(starts), parents=parents),
        out_shape=jax.ShapeDtypeStruct((leaves, n, size), BF16),
        grid_spec=pltpu.PrefetchScalarGridSpec(
            num_scalar_prefetch=3,
            grid=(steps,),
            in_specs=[pl.BlockSpec(memory_space=pl.ANY) for _ in blocks]
            + [
                pl.BlockSpec((pc,) + coupling.shape[1:], at3),
                pl.BlockSpec((pc,) + transfer.shape[1:], at3),
                pl.BlockSpec((lc,) + basis.shape[1:], at3),
                pl.BlockSpec((lc, n, size), at3),
                pl.BlockSpec((pc,) + field.shape[1:], at3),
            ],
            out_specs=pl.BlockSpec((lc, n, size), at3),
            scratch_shapes=[
                pltpu.VMEM((devices * parents,) + blocks[0].shape[1:], BF16),
                pltpu.SemaphoreType.DMA((len(blocks),)),
            ],
        ),
        name="downward",
    )(me, owner, local, *blocks, coupling, transfer, basis, near, field)


def on_device(
    points_rhs,
    leaf_basis,
    transfer,
    leaf_coupling,
    parent_coupling,
    near_blocks,
    near_offsets,
    coupling_offsets,
    parent_owner,
    parent_local,
):
    streams, leafs = lax.axis_size("stream"), lax.axis_size("leaf")
    devices = streams * leafs
    parents = transfer.shape[0]
    me = lax.axis_index(AXES).astype(jnp.int32)
    par = (me % 2).reshape(1)

    def swap(x, bits):
        return lax.ppermute(x, AXES, [(i, i ^ bits) for i in range(devices)])

    coeffs, payload, side = upward(par, points_rhs, leaf_basis, transfer)
    odd_pairs = [(i, i + 1) for i in range(1, devices - 1, 2)]
    side_in = lax.ppermute(side, AXES, odd_pairs + [(b, a) for a, b in odd_pairs])

    got = swap(payload, 1)
    groups = []
    group = jnp.concatenate([payload[:parents], got[:parents]], axis=0)
    groups.append((0, group))
    bit = 2
    while bit < leafs:
        whole = jnp.concatenate([g for _, g in groups], axis=0)
        groups.append((bit, swap(whole, bit)))
        bit *= 2

    blocks, starts = [], []
    for base, group in groups:
        have = {0: group}
        for s in range(2, streams, 2):
            low = s & -s
            high = 1 << (s.bit_length() - 1)
            if low == high:
                have[s] = swap(have[s ^ low], s * leafs)
            else:
                rows = group.shape[0] // 2
                have[s] = jnp.concatenate(
                    [swap(have[s ^ low][:rows], low * leafs), swap(have[s ^ high][rows:], high * leafs)], axis=0
                )
        for s in list(have):
            have[s ^ 1] = swap(have[s], leafs)
        for s, g in have.items():
            blocks.append(g)
            starts.append((s * leafs + base) * parents)

    near, field = local_terms(
        par, near_offsets, coupling_offsets, points_rhs, coeffs, got, side_in, near_blocks, leaf_coupling
    )
    return downward(
        me.reshape(1), parent_owner, parent_local, blocks, starts,
        parent_coupling, transfer, leaf_basis, near, field, devices,
    )


def solution(mesh):
    three = P(AXES, None, None)
    two = P(AXES, None)
    return jax.shard_map(
        on_device,
        mesh=mesh,
        in_specs=(three,) * 5 + (P(AXES, None, None, None),) + (two,) * 4,
        out_specs=three,
        check_vma=False,
    )
```

```python
import functools

import jax
import jax.numpy as jnp
from jax import lax
from jax.experimental import pallas as pl
from jax.experimental.pallas import tpu as pltpu
from jax.sharding import PartitionSpec as P

AXES = ("stream", "leaf")
FAR = 5
NEAR = 2
F32 = jnp.float32
BF16 = jnp.bfloat16

LIMIT = 16 * 1024 * 1024


def dot_t(a, b):
    return lax.dot_general(a, b, (((1,), (1,)), ((), ())), preferred_element_type=F32)


def dot_n(a, b):
    return lax.dot_general(a, b, (((1,), (0,)), ((), ())), preferred_element_type=F32)


def in_hbm(x):
    return pltpu.with_memory_space_constraint(x, pltpu.HBM)


def left_half(rows, lanes):
    return lax.broadcasted_iota(jnp.int32, (rows, lanes), 1) < lanes // 2


def swap_halves(tile):
    half = tile.shape[1] // 2
    return jnp.concatenate([tile[:, half:], tile[:, :half]], axis=1)


def beside(tiles, mask):
    tops, bots = [], []
    for a, b in zip(tiles[::2], tiles[1::2]):
        tops.append(jnp.where(mask, a, swap_halves(b)))
        bots.append(jnp.where(mask, swap_halves(a), b))
    return jnp.concatenate([jnp.concatenate(tops, axis=1), jnp.concatenate(bots, axis=1)], axis=0)


def dense(doubled, mask):
    half = doubled.shape[0] // 2
    return jnp.where(mask, doubled[:half], doubled[half:]).astype(BF16)


def upward_kernel(par_ref, pts_ref, basis_ref, trans_ref, coeff_ref, pay_ref, side_ref, *, steps, parents):
    step = pl.program_id(0)
    pairs = trans_ref.shape[0]
    n = pts_ref.shape[1]
    wide = left_half(n, 128)
    mask = left_half(n // 2, 128)
    batch = 4
    for first in range(0, pairs, batch):
        own = range(first, first + batch)
        sums = []
        for leaf in range(2 * first, 2 * (first + batch)):
            b = basis_ref[leaf]
            sums.append(dot_t(pts_ref[leaf], jnp.concatenate([b, b], axis=0)))
        paired = [jnp.where(wide, sums[2 * q], sums[2 * q + 1]).astype(BF16) for q in range(batch)]
        ups = []
        for q, p in enumerate(own):
            t = trans_ref[p]
            ups.append(dot_t(paired[q], jnp.concatenate([t, t], axis=0)))
        for q, c in enumerate(sums):
            coeff_ref[2 * first + q] = dense(c, mask)
        for q, p in enumerate(own):
            pay_ref[step * pairs + p] = dense(ups[q], mask)

    def edge(ref, at, first):
        leaves = pts_ref.shape[0]
        lo = 0 if first else leaves - FAR
        for q in range(FAR):
            ref[at + q] = coeff_ref[lo + q]
        lo = 0 if first else leaves - NEAR
        for q in range(NEAR):
            x = pts_ref[lo + q]
            ref[at + FAR + 2 * q] = x[: n // 2]
            ref[at + FAR + 2 * q + 1] = x[n // 2 :]

    odd = par_ref[0] == 1

    @pl.when(step == 0)
    def _():
        @pl.when(odd)
        def _():
            edge(pay_ref, parents, True)

        @pl.when(jnp.logical_not(odd))
        def _():
            edge(side_ref, 0, True)

    @pl.when(step == steps - 1)
    def _():
        @pl.when(odd)
        def _():
            edge(side_ref, 0, False)

        @pl.when(jnp.logical_not(odd))
        def _():
            edge(pay_ref, parents, False)


def upward(par, points, basis, transfer):
    leaves, n, size = points.shape
    parents, rank, _ = transfer.shape
    steps = 4
    lc, pc = leaves // steps, parents // steps
    halo = FAR + 2 * NEAR
    tile = (n // 2, 2 * rank)
    return pl.pallas_call(
        functools.partial(upward_kernel, steps=steps, parents=parents),
        out_shape=(
            jax.ShapeDtypeStruct((leaves,) + tile, BF16),
            jax.ShapeDtypeStruct((parents + halo,) + tile, BF16),
            jax.ShapeDtypeStruct((halo,) + tile, BF16),
        ),
        grid_spec=pltpu.PrefetchScalarGridSpec(
            num_scalar_prefetch=1,
            grid=(steps,),
            in_specs=[
                pl.BlockSpec((lc, n, size), lambda i, s: (i, 0, 0)),
                pl.BlockSpec((lc, rank, size), lambda i, s: (i, 0, 0)),
                pl.BlockSpec((pc, rank, 2 * rank), lambda i, s: (i, 0, 0)),
            ],
            out_specs=[
                pl.BlockSpec((lc,) + tile, lambda i, s: (i, 0, 0)),
                pl.BlockSpec((parents + halo,) + tile, lambda i, s: (0, 0, 0)),
                pl.BlockSpec((halo,) + tile, lambda i, s: (0, 0, 0)),
            ],
        ),
        compiler_params=pltpu.CompilerParams(vmem_limit_bytes=LIMIT),
        name="upward",
    )(par, *[in_hbm(x) for x in (points, basis, transfer)])


def local_kernel(
    par_ref, noff_ref, coff_ref, pts_ref, coeff_ref, pay_ref, side_ref, near_ref, coup_ref,
    near_out, field_out, pts_pad, coeff_pad, *, parents
):
    step = pl.program_id(0)
    leaves = pts_ref.shape[0]
    n = pts_ref.shape[1]
    chunk = near_ref.shape[0]
    mask = left_half(n // 2, 128)
    wide = left_half(n, 128)

    @pl.when(step == 0)
    def _():
        pts_pad[NEAR : NEAR + leaves] = pts_ref[...]
        coeff_pad[FAR : FAR + leaves] = coeff_ref[...]

        def put(ref, at, low):
            co = 0 if low else leaves + FAR
            po = 0 if low else leaves + NEAR
            for q in range(FAR):
                coeff_pad[co + q] = ref[at + q]
            for q in range(NEAR):
                pts_pad[po + q, : n // 2] = ref[at + FAR + 2 * q]
                pts_pad[po + q, n // 2 :] = ref[at + FAR + 2 * q + 1]

        odd = par_ref[0] == 1

        @pl.when(odd)
        def _():
            put(pay_ref, parents, True)
            put(side_ref, 0, False)

        @pl.when(jnp.logical_not(odd))
        def _():
            put(side_ref, 0, True)
            put(pay_ref, parents, False)

    slots = near_ref.shape[1]
    far_slots = coff_ref.shape[0]
    batch = 4
    for first in range(0, chunk, batch):
        nears, fields = [], []
        for j in range(first, first + batch):
            c = step * chunk + j
            xs = [pts_pad[c + NEAR + noff_ref[k, c]] for k in range(slots)]
            ws = [near_ref[j, k] for k in range(slots)]
            nears.append(dot_t(jnp.concatenate(xs, axis=1), jnp.concatenate(ws, axis=1)))
            w = coup_ref[j]
            lhs = beside([coeff_pad[c + FAR + coff_ref[k, c]] for k in range(far_slots)], mask)
            fields.append(dot_t(lhs, jnp.concatenate([w, w], axis=0)))
        for q, j in enumerate(range(first, first + batch)):
            near_out[j] = nears[q]
        for q in range(0, batch, 2):
            field_out[(first + q) // 2] = jnp.where(wide, fields[q], fields[q + 1])


def local_terms(par, near_offsets, coupling_offsets, points, coeffs, payload, side, near_blocks, leaf_coupling):
    leaves, n, size = points.shape
    rank = leaf_coupling.shape[1]
    slots = near_blocks.shape[1]
    chunk = 8
    halo = side.shape[0]
    parents = payload.shape[0] - halo
    tile = side.shape[1:]
    whole = lambda i, *s: (0, 0, 0)
    return pl.pallas_call(
        functools.partial(local_kernel, parents=parents),
        out_shape=(
            jax.ShapeDtypeStruct((leaves, n, size), F32),
            jax.ShapeDtypeStruct((leaves // 2, n, 2 * rank), F32),
        ),
        grid_spec=pltpu.PrefetchScalarGridSpec(
            num_scalar_prefetch=3,
            grid=(leaves // chunk,),
            in_specs=[
                pl.BlockSpec(points.shape, whole),
                pl.BlockSpec(coeffs.shape, whole),
                pl.BlockSpec(payload.shape, whole),
                pl.BlockSpec(side.shape, whole),
                pl.BlockSpec((chunk, slots, size, size), lambda i, *s: (i, 0, 0, 0)),
                pl.BlockSpec((chunk,) + leaf_coupling.shape[1:], lambda i, *s: (i, 0, 0)),
            ],
            out_specs=[
                pl.BlockSpec((chunk, n, size), lambda i, *s: (i, 0, 0)),
                pl.BlockSpec((chunk // 2, n, 2 * rank), lambda i, *s: (i, 0, 0)),
            ],
            scratch_shapes=[
                pltpu.VMEM((leaves + 2 * NEAR, n, size), BF16),
                pltpu.VMEM((leaves + 2 * FAR,) + tile, BF16),
            ],
        ),
        compiler_params=pltpu.CompilerParams(vmem_limit_bytes=LIMIT),
        name="local_terms",
    )(
        par, near_offsets, coupling_offsets, points, coeffs, payload, side, in_hbm(near_blocks), in_hbm(leaf_coupling)
    )


def downward_kernel(
    me_ref, owner_ref, local_ref, table, coup_ref, trans_ref, basis_ref, near_ref, field_ref, out_ref
):
    parents = trans_ref.shape[0]
    n = near_ref.shape[1]
    size = near_ref.shape[2]
    slots = owner_ref.shape[0]
    mask = left_half(n // 2, 128)
    zero = jnp.zeros(basis_ref.shape[1:], BF16)
    me = me_ref[0]
    batch = 4

    def rows(step, carry):
        own = [step * batch + q for q in range(batch)]
        halves = []
        for p in own:
            tiles = [table[(owner_ref[k, p] ^ me) * parents + local_ref[k, p]] for k in range(slots)]
            halves.append(dot_t(beside(tiles, mask), coup_ref[p]).astype(BF16))
        totals = [
            (field_ref[p] + dot_n(half, trans_ref[p])).astype(BF16) for p, half in zip(own, halves)
        ]
        fars = []
        for p, total in zip(own, totals):
            spread = jnp.concatenate(
                [
                    jnp.concatenate([basis_ref[2 * p], zero], axis=1),
                    jnp.concatenate([zero, basis_ref[2 * p + 1]], axis=1),
                ],
                axis=0,
            )
            fars.append(dot_n(total, spread))
        outs = []
        for p, far in zip(own, fars):
            outs.append((far[:, :size] + near_ref[2 * p]).astype(BF16))
            outs.append((far[:, size:] + near_ref[2 * p + 1]).astype(BF16))
        for q, out in enumerate(outs):
            out_ref[2 * batch * step + q] = out
        return carry

    lax.fori_loop(0, parents // batch, rows, 0)


def downward(me, owner, local, table, coupling, transfer, basis, near, field):
    leaves, n, size = near.shape
    smem = pl.BlockSpec(memory_space=pltpu.SMEM)
    vmem = pl.BlockSpec(memory_space=pltpu.VMEM)
    big = [pltpu.with_memory_space_constraint(x, pltpu.VMEM) for x in (table, coupling, transfer, basis, near, field)]
    return pl.pallas_call(
        downward_kernel,
        out_shape=jax.ShapeDtypeStruct((leaves, n, size), BF16),
        in_specs=[smem] * 3 + [vmem] * 6,
        out_specs=vmem,
        compiler_params=pltpu.CompilerParams(vmem_limit_bytes=LIMIT),
        name="downward",
    )(me, owner, local, *big)


def on_device(
    points_rhs,
    leaf_basis,
    transfer,
    leaf_coupling,
    parent_coupling,
    near_blocks,
    near_offsets,
    coupling_offsets,
    parent_owner,
    parent_local,
):
    streams, leafs = lax.axis_size("stream"), lax.axis_size("leaf")
    devices = streams * leafs
    parents = transfer.shape[0]
    me = lax.axis_index(AXES).astype(jnp.int32)
    par = (me % 2).reshape(1)

    def swap(x, bits):
        return lax.ppermute(x, AXES, [(i, i ^ bits) for i in range(devices)])

    coeffs, payload, side = upward(par, points_rhs, leaf_basis, transfer)
    odd_pairs = [(i, i + 1) for i in range(1, devices - 1, 2)]
    side_in = lax.ppermute(side, AXES, odd_pairs + [(b, a) for a, b in odd_pairs])

    got = swap(payload, 1)
    groups = []
    group = jnp.concatenate([payload[:parents], got[:parents]], axis=0)
    groups.append((0, group))
    bit = 2
    while bit < leafs:
        whole = jnp.concatenate([g for _, g in groups], axis=0)
        groups.append((bit, swap(whole, bit)))
        bit *= 2

    pieces = {}
    for base, group in groups:
        have = {0: group}
        for s in range(2, streams, 2):
            low = s & -s
            high = 1 << (s.bit_length() - 1)
            if low == high:
                have[s] = swap(have[s ^ low], s * leafs)
            else:
                rows = group.shape[0] // 2
                have[s] = jnp.concatenate(
                    [swap(have[s ^ low][:rows], low * leafs), swap(have[s ^ high][rows:], high * leafs)],
                    axis=0,
                )
        for s in list(have):
            have[s ^ 1] = swap(have[s], leafs)
        for s, g in have.items():
            pieces[s * leafs + base] = g
    table = jnp.concatenate([pieces[k] for k in sorted(pieces)], axis=0)

    near, field = local_terms(
        par, near_offsets.T, coupling_offsets.T, points_rhs, coeffs, got, side_in, near_blocks, leaf_coupling
    )
    return downward(
        me.reshape(1), parent_owner.T, parent_local.T, table, parent_coupling, transfer, leaf_basis, near, field
    )


def solution(mesh):
    three = P(AXES, None, None)
    two = P(AXES, None)
    return jax.shard_map(
        on_device,
        mesh=mesh,
        in_specs=(three,) * 5 + (P(AXES, None, None, None),) + (two,) * 4,
        out_specs=three,
        check_vma=False,
    )
```

```python
import functools

import jax
import jax.numpy as jnp
from jax import lax
from jax.experimental import pallas as pl
from jax.experimental.pallas import tpu as pltpu
from jax.sharding import PartitionSpec as P


AXES = ("stream", "leaf")
FAR = 5
NEAR = 2
F32 = jnp.float32
BF16 = jnp.bfloat16

AHEAD = 3
LIMIT = 16 * 1024 * 1024


def dot_t(a, b):
    return lax.dot_general(a, b, (((1,), (1,)), ((), ())), preferred_element_type=F32)


def dot_n(a, b):
    return lax.dot_general(a, b, (((1,), (0,)), ((), ())), preferred_element_type=F32)


def in_hbm(x):
    return pltpu.with_memory_space_constraint(x, pltpu.HBM)


def left_half(rows, lanes):
    return lax.broadcasted_iota(jnp.int32, (rows, lanes), 1) < lanes // 2


def swap_halves(tile):
    half = tile.shape[1] // 2
    return jnp.concatenate([tile[:, half:], tile[:, :half]], axis=1)


def beside(tiles, mask):
    tops, bots = [], []
    for a, b in zip(tiles[::2], tiles[1::2]):
        tops.append(jnp.where(mask, a, swap_halves(b)))
        bots.append(jnp.where(mask, swap_halves(a), b))
    return jnp.concatenate([jnp.concatenate(tops, axis=1), jnp.concatenate(bots, axis=1)], axis=0)


def dense(pair, mask):
    half = pair.shape[0] // 2
    top, bot = pair[:half], pair[half:]
    return jnp.where(mask, top, swap_halves(bot)), jnp.where(mask, swap_halves(top), bot)


def diagonal(a, b):
    zero = jnp.zeros_like(a)
    return jnp.concatenate(
        [jnp.concatenate([a, zero], axis=1), jnp.concatenate([zero, b], axis=1)], axis=0
    )


def upward_kernel(
    par_ref, pts_hbm, basis_hbm, trans_hbm, coeff_ref, pay_ref, side_ref, pts_ref, basis_ref, trans_ref, sems, *, steps
):
    leaves, n, _ = pts_ref.shape
    parents = trans_ref.shape[0]
    mask = left_half(n // 2, 128)
    pairs = parents // steps

    def copies(i):
        own = pl.ds(i * pairs, pairs)
        both = pl.ds(2 * i * pairs, 2 * pairs)
        return (
            pltpu.make_async_copy(pts_hbm.at[both], pts_ref.at[both], sems.at[0, i]),
            pltpu.make_async_copy(basis_hbm.at[both], basis_ref.at[both], sems.at[1, i]),
            pltpu.make_async_copy(trans_hbm.at[own], trans_ref.at[own], sems.at[2, i]),
        )

    for i in range(steps):
        for c in copies(i):
            c.start()

    for i in range(steps):
        for c in copies(i):
            c.wait()
        own = range(i * pairs, (i + 1) * pairs)
        paired = []
        for p in own:
            x = jnp.concatenate([pts_ref[2 * p], pts_ref[2 * p + 1]], axis=1)
            paired.append(dot_t(x, diagonal(basis_ref[2 * p], basis_ref[2 * p + 1])).astype(BF16))
        ups = []
        for q in range(0, pairs, 2):
            x = jnp.concatenate([paired[q], paired[q + 1]], axis=1)
            ups.append(dot_t(x, diagonal(trans_ref[own[q]], trans_ref[own[q + 1]])).astype(BF16))
        for q, p in enumerate(own):
            coeff_ref[2 * p], coeff_ref[2 * p + 1] = dense(paired[q], mask)
        for q, up in enumerate(ups):
            p = own[2 * q]
            pay_ref[p], pay_ref[p + 1] = dense(up, mask)

    def edge(ref, at, first):
        lo = 0 if first else leaves - FAR
        for q in range(FAR):
            ref[at + q] = coeff_ref[lo + q]
        lo = 0 if first else leaves - NEAR
        for q in range(NEAR):
            x = pts_ref[lo + q]
            ref[at + FAR + 2 * q] = x[: n // 2]
            ref[at + FAR + 2 * q + 1] = x[n // 2 :]

    odd = par_ref[0] == 1

    @pl.when(odd)
    def _():
        edge(pay_ref, parents, True)
        edge(side_ref, 0, False)

    @pl.when(jnp.logical_not(odd))
    def _():
        edge(side_ref, 0, True)
        edge(pay_ref, parents, False)


def upward(par, points, basis, transfer):
    leaves, n, _ = points.shape
    parents, rank, _ = transfer.shape
    steps = 2
    halo = FAR + 2 * NEAR
    tile = (n // 2, 2 * rank)
    smem = pl.BlockSpec(memory_space=pltpu.SMEM)
    vmem = pl.BlockSpec(memory_space=pltpu.VMEM)
    hbm = pl.BlockSpec(memory_space=pltpu.HBM)
    return pl.pallas_call(
        functools.partial(upward_kernel, steps=steps),
        out_shape=(
            jax.ShapeDtypeStruct((leaves,) + tile, BF16),
            jax.ShapeDtypeStruct((parents + halo,) + tile, BF16),
            jax.ShapeDtypeStruct((halo,) + tile, BF16),
        ),
        in_specs=[smem] + [hbm] * 3,
        out_specs=[vmem] * 3,
        scratch_shapes=[
            pltpu.VMEM(points.shape, BF16),
            pltpu.VMEM(basis.shape, BF16),
            pltpu.VMEM(transfer.shape, BF16),
            pltpu.SemaphoreType.DMA((3, steps)),
        ],
        compiler_params=pltpu.CompilerParams(vmem_limit_bytes=LIMIT),
        name="upward",
    )(par, *[in_hbm(x) for x in (points, basis, transfer)])


def local_kernel(
    par_ref, noff_ref, coff_ref, pts_hbm, near_hbm, coup_hbm, coeff_ref, pay_ref, side_ref,
    near_out, field_out, pts_pad, coeff_pad, near_ref, coup_ref, sems, pts_sem, *, steps
):
    leaves, n, _ = pts_hbm.shape
    chunk = leaves // steps
    slots = near_ref.shape[1]
    far_slots = coff_ref.shape[0]
    halo = side_ref.shape[0]
    at = pay_ref.shape[0] - halo
    mask = left_half(n // 2, 128)

    def copies(i):
        own = pl.ds(i * chunk, chunk)
        return (
            pltpu.make_async_copy(near_hbm.at[own], near_ref.at[own], sems.at[0, i]),
            pltpu.make_async_copy(coup_hbm.at[own], coup_ref.at[own], sems.at[1, i]),
        )

    points_in = pltpu.make_async_copy(pts_hbm, pts_pad.at[pl.ds(NEAR, leaves)], pts_sem)
    points_in.start()
    for i in range(AHEAD):
        for c in copies(i):
            c.start()

    coeff_pad[FAR : FAR + leaves] = coeff_ref[...]

    def put(ref, at, low):
        co = 0 if low else leaves + FAR
        po = 0 if low else leaves + NEAR
        for q in range(FAR):
            coeff_pad[co + q] = ref[at + q]
        for q in range(NEAR):
            pts_pad[po + q, : n // 2] = ref[at + FAR + 2 * q]
            pts_pad[po + q, n // 2 :] = ref[at + FAR + 2 * q + 1]

    odd = par_ref[0] == 1

    @pl.when(odd)
    def _():
        put(pay_ref, at, True)
        put(side_ref, 0, False)

    @pl.when(jnp.logical_not(odd))
    def _():
        put(side_ref, 0, True)
        put(pay_ref, at, False)

    points_in.wait()

    def body(i, carry):
        for c in copies(i):
            c.wait()

        @pl.when(i + AHEAD < steps)
        def _():
            for c in copies(i + AHEAD):
                c.start()

        nears, fields = [], []
        for j in range(chunk):
            c = i * chunk + j
            xs = [pts_pad[c + NEAR + noff_ref[k, c]] for k in range(slots)]
            ws = [near_ref[c, k] for k in range(slots)]
            nears.append(dot_t(jnp.concatenate(xs, axis=1), jnp.concatenate(ws, axis=1)))
        for j in range(chunk):
            c = i * chunk + j
            lhs = beside([coeff_pad[c + FAR + coff_ref[k, c]] for k in range(far_slots)], mask)
            fields.append(dot_t(lhs, coup_ref[c]))
        for j in range(chunk):
            near_out[i * chunk + j] = nears[j]
        for j in range(0, chunk, 2):
            field_out[(i * chunk + j) // 2] = jnp.concatenate([fields[j], fields[j + 1]], axis=1)
        return carry

    lax.fori_loop(0, steps, body, 0)


def local_terms(par, near_offsets, coupling_offsets, points, coeffs, payload, side, near_blocks, leaf_coupling):
    leaves, n, size = points.shape
    rank = leaf_coupling.shape[1]
    steps = 8
    tile = side.shape[1:]
    smem = pl.BlockSpec(memory_space=pltpu.SMEM)
    vmem = pl.BlockSpec(memory_space=pltpu.VMEM)
    hbm = pl.BlockSpec(memory_space=pltpu.HBM)
    return pl.pallas_call(
        functools.partial(local_kernel, steps=steps),
        out_shape=(
            jax.ShapeDtypeStruct((leaves, n, size), F32),
            jax.ShapeDtypeStruct((leaves // 2, n, 2 * rank), F32),
        ),
        in_specs=[smem] * 3 + [hbm] * 3 + [vmem] * 3,
        out_specs=[vmem] * 2,
        scratch_shapes=[
            pltpu.VMEM((leaves + 2 * NEAR, n, size), BF16),
            pltpu.VMEM((leaves + 2 * FAR,) + tile, BF16),
            pltpu.VMEM(near_blocks.shape, BF16),
            pltpu.VMEM(leaf_coupling.shape, BF16),
            pltpu.SemaphoreType.DMA((2, steps)),
            pltpu.SemaphoreType.DMA,
        ],
        compiler_params=pltpu.CompilerParams(vmem_limit_bytes=LIMIT),
        name="local_terms",
    )(
        par, near_offsets, coupling_offsets, in_hbm(points), in_hbm(near_blocks), in_hbm(leaf_coupling),
        coeffs, payload, side,
    )


def downward_kernel(
    me_ref, owner_ref, local_ref, table, coup_ref, trans_ref, basis_ref, near_ref, field_ref, out_hbm, out_ref, sems,
    *, batch
):
    parents = trans_ref.shape[0]
    n = near_ref.shape[1]
    size = near_ref.shape[2]
    slots = owner_ref.shape[0]
    mask = left_half(n // 2, 128)
    me = me_ref[0]

    def copy(step):
        own = pl.ds(2 * batch * step, 2 * batch)
        return pltpu.make_async_copy(out_ref.at[own], out_hbm.at[own], sems.at[step])

    def rows(step, carry):
        own = [step * batch + q for q in range(batch)]
        halves = []
        for p in own:
            tiles = [table[(owner_ref[k, p] ^ me) * parents + local_ref[k, p]] for k in range(slots)]
            halves.append(dot_t(beside(tiles, mask), coup_ref[p]).astype(BF16))
        totals = [
            (field_ref[p] + dot_n(half, trans_ref[p])).astype(BF16) for p, half in zip(own, halves)
        ]
        fars = []
        for p, total in zip(own, totals):
            spread = diagonal(basis_ref[2 * p], basis_ref[2 * p + 1])
            fars.append(dot_n(total, spread))
        outs = []
        for p, far in zip(own, fars):
            outs.append((far[:, :size] + near_ref[2 * p]).astype(BF16))
            outs.append((far[:, size:] + near_ref[2 * p + 1]).astype(BF16))
        for q, out in enumerate(outs):
            out_ref[2 * batch * step + q] = out
        copy(step).start()
        return carry

    lax.fori_loop(0, parents // batch, rows, 0)
    for step in range(parents // batch):
        copy(step).wait()


def downward(me, owner, local, table, coupling, transfer, basis, near, field):
    leaves, n, size = near.shape
    smem = pl.BlockSpec(memory_space=pltpu.SMEM)
    vmem = pl.BlockSpec(memory_space=pltpu.VMEM)
    big = [pltpu.with_memory_space_constraint(x, pltpu.VMEM) for x in (table, coupling, transfer, basis, near, field)]
    batch = 8
    return pl.pallas_call(
        functools.partial(downward_kernel, batch=batch),
        out_shape=jax.ShapeDtypeStruct((leaves, n, size), BF16),
        in_specs=[smem] * 3 + [vmem] * 6,
        out_specs=pl.BlockSpec(memory_space=pltpu.HBM),
        scratch_shapes=[
            pltpu.VMEM((leaves, n, size), BF16),
            pltpu.SemaphoreType.DMA((transfer.shape[0] // batch,)),
        ],
        compiler_params=pltpu.CompilerParams(vmem_limit_bytes=LIMIT),
        name="downward",
    )(me, owner, local, *big)


def on_device(
    points_rhs,
    leaf_basis,
    transfer,
    leaf_coupling,
    parent_coupling,
    near_blocks,
    near_offsets,
    coupling_offsets,
    parent_owner,
    parent_local,
):
    streams, leafs = lax.axis_size("stream"), lax.axis_size("leaf")
    devices = streams * leafs
    parents = transfer.shape[0]
    me = lax.axis_index(AXES).astype(jnp.int32)
    par = (me % 2).reshape(1)

    def swap(x, bits):
        return lax.ppermute(x, AXES, [(i, i ^ bits) for i in range(devices)])

    coeffs, payload, side = upward(par, points_rhs, leaf_basis, transfer)
    odd_pairs = [(i, i + 1) for i in range(1, devices - 1, 2)]
    side_in = lax.ppermute(side, AXES, odd_pairs + [(b, a) for a, b in odd_pairs])

    got = swap(payload, 1)
    line = [payload[:parents], got[:parents]]
    line += [swap(line[0], k) for k in range(2, leafs)]
    groups = [(0, jnp.concatenate(line[:2], axis=0)), (2, jnp.concatenate(line[2:], axis=0))]

    pieces = {}
    for base, group in groups:
        have = {0: group}
        for s in range(2, streams, 2):
            low = s & -s
            high = 1 << (s.bit_length() - 1)
            if low == high:
                have[s] = swap(have[s ^ low], s * leafs)
            else:
                rows = group.shape[0] // 2
                have[s] = jnp.concatenate(
                    [swap(have[s ^ low][:rows], low * leafs), swap(have[s ^ high][rows:], high * leafs)],
                    axis=0,
                )
        for s in list(have):
            have[s ^ 1] = swap(have[s], leafs)
        for s, g in have.items():
            pieces[s * leafs + base] = g
    table = jnp.concatenate([pieces[k] for k in sorted(pieces)], axis=0)

    near, field = local_terms(
        par, near_offsets.T, coupling_offsets.T, points_rhs, coeffs, got, side_in, near_blocks, leaf_coupling
    )
    return downward(
        me.reshape(1), parent_owner.T, parent_local.T, table, parent_coupling, transfer, leaf_basis, near, field
    )


def solution(mesh):
    three = P(AXES, None, None)
    two = P(AXES, None)
    return jax.shard_map(
        on_device,
        mesh=mesh,
        in_specs=(three,) * 5 + (P(AXES, None, None, None),) + (two,) * 4,
        out_specs=three,
        check_vma=False,
    )
```

```python
import functools

import jax
import jax.numpy as jnp
from jax import lax
from jax.experimental import pallas as pl
from jax.experimental.pallas import tpu as pltpu
from jax.sharding import PartitionSpec as P


AXES = ("stream", "leaf")
FAR = 5
NEAR = 2
F32 = jnp.float32
BF16 = jnp.bfloat16

AHEAD = 2
LIMIT = 16 * 1024 * 1024


def dot_t(a, b):
    return lax.dot_general(a, b, (((1,), (1,)), ((), ())), preferred_element_type=F32)


def dot_n(a, b):
    return lax.dot_general(a, b, (((1,), (0,)), ((), ())), preferred_element_type=F32)


def in_hbm(x):
    return pltpu.with_memory_space_constraint(x, pltpu.HBM)


def left_half(rows, lanes):
    return lax.broadcasted_iota(jnp.int32, (rows, lanes), 1) < lanes // 2


def swap_halves(tile):
    half = tile.shape[1] // 2
    return jnp.concatenate([tile[:, half:], tile[:, :half]], axis=1)


def beside(tiles, mask):
    tops, bots = [], []
    for a, b in zip(tiles[::2], tiles[1::2]):
        tops.append(jnp.where(mask, a, swap_halves(b)))
        bots.append(jnp.where(mask, swap_halves(a), b))
    return jnp.concatenate([jnp.concatenate(tops, axis=1), jnp.concatenate(bots, axis=1)], axis=0)


def dense(pair, mask):
    half = pair.shape[0] // 2
    top, bot = pair[:half], pair[half:]
    return jnp.where(mask, top, swap_halves(bot)), jnp.where(mask, swap_halves(top), bot)


def diagonal(a, b):
    zero = jnp.zeros_like(a)
    return jnp.concatenate(
        [jnp.concatenate([a, zero], axis=1), jnp.concatenate([zero, b], axis=1)], axis=0
    )


def upward_kernel(
    me_ref, pts_hbm, basis_hbm, trans_hbm, coeff_ref, pay_ref, side_ref, pts_ref, basis_ref, trans_ref, sems, *, steps
):
    leaves, n, _ = pts_ref.shape
    parents = trans_ref.shape[0]
    mask = left_half(n // 2, 128)
    pairs = parents // steps

    def copies(i):
        own = pl.ds(i * pairs, pairs)
        both = pl.ds(2 * i * pairs, 2 * pairs)
        return (
            pltpu.make_async_copy(pts_hbm.at[both], pts_ref.at[both], sems.at[0, i]),
            pltpu.make_async_copy(basis_hbm.at[both], basis_ref.at[both], sems.at[1, i]),
            pltpu.make_async_copy(trans_hbm.at[own], trans_ref.at[own], sems.at[2, i]),
        )

    for i in range(steps):
        for c in copies(i):
            c.start()

    for i in range(steps):
        for c in copies(i):
            c.wait()
        own = range(i * pairs, (i + 1) * pairs)
        paired = []
        for p in own:
            x = jnp.concatenate([pts_ref[2 * p], pts_ref[2 * p + 1]], axis=1)
            paired.append(dot_t(x, diagonal(basis_ref[2 * p], basis_ref[2 * p + 1])).astype(BF16))
        ups = []
        for q in range(0, pairs, 2):
            x = jnp.concatenate([paired[q], paired[q + 1]], axis=1)
            ups.append(dot_t(x, diagonal(trans_ref[own[q]], trans_ref[own[q + 1]])).astype(BF16))
        for q, p in enumerate(own):
            coeff_ref[2 * p], coeff_ref[2 * p + 1] = dense(paired[q], mask)
        for q, up in enumerate(ups):
            p = own[2 * q]
            pay_ref[p], pay_ref[p + 1] = dense(up, mask)

    def edge(ref, at, first):
        lo = 0 if first else leaves - FAR
        for q in range(FAR):
            ref[at + q] = coeff_ref[lo + q]
        lo = 0 if first else leaves - NEAR
        for q in range(NEAR):
            x = pts_ref[lo + q]
            ref[at + FAR + 2 * q] = x[: n // 2]
            ref[at + FAR + 2 * q + 1] = x[n // 2 :]

    odd = me_ref[0] & 1 == 1

    @pl.when(odd)
    def _():
        edge(pay_ref, parents, True)
        edge(side_ref, 0, False)

    @pl.when(jnp.logical_not(odd))
    def _():
        edge(side_ref, 0, True)
        edge(pay_ref, parents, False)


def upward(me, points, basis, transfer):
    leaves, n, _ = points.shape
    parents, rank, _ = transfer.shape
    steps = 2
    halo = FAR + 2 * NEAR
    tile = (n // 2, 2 * rank)
    smem = pl.BlockSpec(memory_space=pltpu.SMEM)
    vmem = pl.BlockSpec(memory_space=pltpu.VMEM)
    hbm = pl.BlockSpec(memory_space=pltpu.HBM)
    return pl.pallas_call(
        functools.partial(upward_kernel, steps=steps),
        out_shape=(
            jax.ShapeDtypeStruct((leaves,) + tile, BF16),
            jax.ShapeDtypeStruct((parents + halo,) + tile, BF16),
            jax.ShapeDtypeStruct((halo,) + tile, BF16),
        ),
        in_specs=[smem] + [hbm] * 3,
        out_specs=[vmem] * 3,
        scratch_shapes=[
            pltpu.VMEM(points.shape, BF16),
            pltpu.VMEM(basis.shape, BF16),
            pltpu.VMEM(transfer.shape, BF16),
            pltpu.SemaphoreType.DMA((3, steps)),
        ],
        compiler_params=pltpu.CompilerParams(vmem_limit_bytes=LIMIT),
        name="upward",
    )(me, *[in_hbm(x) for x in (points, basis, transfer)])


def local_kernel(
    me_ref, noff_hbm, coff_hbm, pts_hbm, near_hbm, coup_hbm, coeff_ref, *refs, leafs, base, stride, edges
):
    if edges:
        pay_ref, side_ref, hop_ref, *refs = refs
    near_out, field_out, noff_ref, coff_ref, pts_pad, coeff_pad, near_ref, coup_ref, sems, first_sems = refs
    leaves, n, _ = pts_hbm.shape
    steps, chunk, slots = near_ref.shape[:3]
    far_slots = coff_ref.shape[0]
    mask = left_half(n // 2, 128)

    def copies(i):
        own = pl.ds(base + stride * i, chunk)
        return (
            pltpu.make_async_copy(near_hbm.at[own], near_ref.at[i], sems.at[0, i]),
            pltpu.make_async_copy(coup_hbm.at[own], coup_ref.at[i], sems.at[1, i]),
        )

    early = (
        pltpu.make_async_copy(noff_hbm, noff_ref, first_sems.at[0]),
        pltpu.make_async_copy(coff_hbm, coff_ref, first_sems.at[1]),
        pltpu.make_async_copy(pts_hbm, pts_pad.at[pl.ds(NEAR, leaves)], first_sems.at[2]),
    )
    for c in early:
        c.start()
    for i in range(min(AHEAD, steps)):
        for c in copies(i):
            c.start()

    coeff_pad[FAR : FAR + leaves] = coeff_ref[...]

    def put(ref, at, low):
        co = 0 if low else leaves + FAR
        po = 0 if low else leaves + NEAR
        for q in range(FAR):
            coeff_pad[co + q] = ref[at + q]
        for q in range(NEAR):
            pts_pad[po + q, : n // 2] = ref[at + FAR + 2 * q]
            pts_pad[po + q, n // 2 :] = ref[at + FAR + 2 * q + 1]

    if edges:
        at = pay_ref.shape[0] - side_ref.shape[0]
        leaf = me_ref[0] & (leafs - 1)
        odd = leaf & 1 == 1

        def put_side(low):
            last = leaf == (0 if low else leafs - 1)

            @pl.when(last)
            def _():
                put(hop_ref, 0, low)

            @pl.when(jnp.logical_not(last))
            def _():
                put(side_ref, 0, low)

        @pl.when(odd)
        def _():
            put(pay_ref, at, True)
            put_side(False)

        @pl.when(jnp.logical_not(odd))
        def _():
            put_side(True)
            put(pay_ref, at, False)

    for c in early:
        c.wait()

    def body(i, carry):
        for c in copies(i):
            c.wait()

        @pl.when(i + AHEAD < steps)
        def _():
            for c in copies(i + AHEAD):
                c.start()

        nears, fields = [], []
        for j in range(chunk):
            c = base + stride * i + j
            xs = [pts_pad[c + NEAR + noff_ref[k, c]] for k in range(slots)]
            ws = [near_ref[i, j, k] for k in range(slots)]
            nears.append(dot_t(jnp.concatenate(xs, axis=1), jnp.concatenate(ws, axis=1)))
        for j in range(chunk):
            c = base + stride * i + j
            lhs = beside([coeff_pad[c + FAR + coff_ref[k, c]] for k in range(far_slots)], mask)
            fields.append(dot_t(lhs, coup_ref[i, j]))
        for j in range(chunk):
            near_out[i * chunk + j] = nears[j]
        for j in range(0, chunk, 2):
            field_out[(i * chunk + j) // 2] = jnp.concatenate([fields[j], fields[j + 1]], axis=1)
        return carry

    lax.fori_loop(0, steps, body, 0)


def local_terms(
    me, near_offsets, coupling_offsets, points, coeffs, halos, near_blocks, leaf_coupling, leafs, base, stride, steps, chunk
):
    leaves, n, size = points.shape
    rank = leaf_coupling.shape[1]
    tile = coeffs.shape[1:]
    smem = pl.BlockSpec(memory_space=pltpu.SMEM)
    vmem = pl.BlockSpec(memory_space=pltpu.VMEM)
    hbm = pl.BlockSpec(memory_space=pltpu.HBM)
    return pl.pallas_call(
        functools.partial(local_kernel, leafs=leafs, base=base, stride=stride, edges=bool(halos)),
        out_shape=(
            jax.ShapeDtypeStruct((steps * chunk, n, size), F32),
            jax.ShapeDtypeStruct((steps * chunk // 2, n, 2 * rank), F32),
        ),
        in_specs=[smem] + [hbm] * 5 + [vmem] * (1 + len(halos)),
        out_specs=[vmem] * 2,
        scratch_shapes=[
            pltpu.SMEM(near_offsets.shape, jnp.int32),
            pltpu.SMEM(coupling_offsets.shape, jnp.int32),
            pltpu.VMEM((leaves + 2 * NEAR, n, size), BF16),
            pltpu.VMEM((leaves + 2 * FAR,) + tile, BF16),
            pltpu.VMEM((steps, chunk) + near_blocks.shape[1:], BF16),
            pltpu.VMEM((steps, chunk) + leaf_coupling.shape[1:], BF16),
            pltpu.SemaphoreType.DMA((2, steps)),
            pltpu.SemaphoreType.DMA((3,)),
        ],
        compiler_params=pltpu.CompilerParams(vmem_limit_bytes=LIMIT),
        name="local_terms",
    )(
        me, *[in_hbm(x) for x in (near_offsets, coupling_offsets, points, near_blocks, leaf_coupling)],
        coeffs, *halos,
    )


def downward_kernel(
    place_hbm, table, coup_ref, trans_ref, basis_ref, near_mid, field_mid, near_rim, field_rim, out_hbm,
    place_ref, out_ref, sems, place_sem, *, batch
):
    parents = trans_ref.shape[0]
    n, size = near_mid.shape[1:]
    slots = place_ref.shape[0]
    mask = left_half(n // 2, 128)
    rim = field_rim.shape[0] // 2
    fetch = pltpu.make_async_copy(place_hbm, place_ref, place_sem)
    fetch.start()
    fetch.wait()

    def run(own, near_ref, field_ref, at):
        halves = []
        for p in own:
            tiles = [table[place_ref[k, p]] for k in range(slots)]
            halves.append(dot_t(beside(tiles, mask), coup_ref[p]).astype(BF16))
        totals = []
        for q, (p, half) in enumerate(zip(own, halves)):
            totals.append((field_ref[at + q] + dot_n(half, trans_ref[p])).astype(BF16))
        fars = []
        for p, total in zip(own, totals):
            fars.append(dot_n(total, diagonal(basis_ref[2 * p], basis_ref[2 * p + 1])))
        for q, (p, far) in enumerate(zip(own, fars)):
            out_ref[2 * p] = (far[:, :size] + near_ref[2 * (at + q)]).astype(BF16)
            out_ref[2 * p + 1] = (far[:, size:] + near_ref[2 * (at + q) + 1]).astype(BF16)

    def copy(first, count, sem):
        own = pl.ds(2 * first, 2 * count)
        return pltpu.make_async_copy(out_ref.at[own], out_hbm.at[own], sem)

    def rows(step, carry):
        first = rim + step * batch
        run([first + q for q in range(batch)], near_mid, field_mid, step * batch)
        copy(first, batch, sems.at[step]).start()
        return carry

    steps = (parents - 2 * rim) // batch
    lax.fori_loop(0, steps, rows, 0)
    run(list(range(rim)) + list(range(parents - rim, parents)), near_rim, field_rim, 0)
    ends = [copy(0, rim, sems.at[steps]), copy(parents - rim, rim, sems.at[steps + 1])]
    for c in ends:
        c.start()
    for step in range(steps):
        copy(rim + step * batch, batch, sems.at[step]).wait()
    for c in ends:
        c.wait()


def downward(place, table, coupling, transfer, basis, mid, rim):
    leaves, _, size = basis.shape
    n = mid[0].shape[1]
    vmem = pl.BlockSpec(memory_space=pltpu.VMEM)
    big = [pltpu.with_memory_space_constraint(x, pltpu.VMEM) for x in (table, coupling, transfer, basis, *mid, *rim)]
    batch = mid[1].shape[0] // 2
    return pl.pallas_call(
        functools.partial(downward_kernel, batch=batch),
        out_shape=jax.ShapeDtypeStruct((leaves, n, size), BF16),
        in_specs=[pl.BlockSpec(memory_space=pl.ANY)] + [vmem] * len(big),
        out_specs=pl.BlockSpec(memory_space=pltpu.HBM),
        scratch_shapes=[
            pltpu.SMEM(place.shape, jnp.int32),
            pltpu.VMEM((leaves, n, size), BF16),
            pltpu.SemaphoreType.DMA((4,)),
            pltpu.SemaphoreType.DMA,
        ],
        compiler_params=pltpu.CompilerParams(vmem_limit_bytes=LIMIT),
        name="downward",
    )(place, *big)


def on_device(
    points_rhs,
    leaf_basis,
    transfer,
    leaf_coupling,
    parent_coupling,
    near_blocks,
    near_offsets,
    coupling_offsets,
    parent_owner,
    parent_local,
):
    streams, leafs = lax.axis_size("stream"), lax.axis_size("leaf")
    devices = streams * leafs
    parents = transfer.shape[0]
    me = lax.axis_index(AXES).astype(jnp.int32)
    flag = me.reshape(1)

    my_leaf = me % leafs

    def permute(x, pairs):
        return lax.ppermute(x, AXES, pairs)

    def swap(x, bits):
        return permute(x, [(i, i ^ bits) for i in range(devices)])

    coeffs, payload, side = upward(flag, points_rhs, leaf_basis, transfer)

    got = swap(payload, 1)
    line = [payload[:parents], got[:parents]]
    sides = None
    for k in range(2, leafs):
        if k & (k + 1):
            line.append(swap(line[0], k))
            continue
        both = swap(jnp.concatenate([line[0], side], axis=0), k)
        line.append(both[:parents])
        if sides is None:
            sides = both[parents:]
        else:
            away = my_leaf ^ jnp.where(my_leaf % 2 == 1, my_leaf + 1, my_leaf - 1)
            sides = jnp.where((away == k) | (k == leafs - 1) & (away > k) | (away < 0), both[parents:], sides)
    ends = [(s * leafs, (s + 1) * leafs) for s in range(streams - 1)]
    ends += [(s * leafs + leafs - 1, s * leafs - 1) for s in range(1, streams)]
    hop = permute(sides, ends)

    groups = [(0, jnp.concatenate(line[:2], axis=0)), (2, jnp.concatenate(line[2:], axis=0))]
    pieces = {}
    for base, group in groups:
        have = {0: group}
        for s in range(2, streams, 2):
            low = s & -s
            high = 1 << (s.bit_length() - 1)
            if low == high:
                have[s] = swap(have[s ^ low], s * leafs)
            else:
                rows = group.shape[0] // 2
                have[s] = jnp.concatenate(
                    [swap(have[s ^ low][:rows], low * leafs), swap(have[s ^ high][rows:], high * leafs)],
                    axis=0,
                )
        for s in list(have):
            have[s ^ 1] = swap(have[s], leafs)
        for s, g in have.items():
            pieces[s * leafs + base] = g
    table = jnp.concatenate([pieces[k] for k in sorted(pieces)], axis=0)

    leaves = points_rhs.shape[0]
    rim = 8
    chunk = (leaves - 2 * rim) // 3
    args = (flag, near_offsets.T, coupling_offsets.T, points_rhs, coeffs)
    mid = local_terms(*args, (), near_blocks, leaf_coupling, leafs, rim, chunk, 3, chunk)
    edge = local_terms(*args, (got, sides, hop), near_blocks, leaf_coupling, leafs, 0, leaves - rim, 2, rim)
    place = (parent_owner.T ^ me) * parents + parent_local.T
    return downward(place, table, parent_coupling, transfer, leaf_basis, mid, edge)


def solution(mesh):
    three = P(AXES, None, None)
    two = P(AXES, None)
    return jax.shard_map(
        on_device,
        mesh=mesh,
        in_specs=(three,) * 5 + (P(AXES, None, None, None),) + (two,) * 4,
        out_specs=three,
        check_vma=False,
    )
```

```python
import functools

import jax
import jax.numpy as jnp
from jax import lax
from jax.experimental import pallas as pl
from jax.experimental.pallas import tpu as pltpu
from jax.sharding import PartitionSpec as P


AXES = ("stream", "leaf")
FAR = 5
NEAR = 2
F32 = jnp.float32
BF16 = jnp.bfloat16

AHEAD = 2
LIMIT = 16 * 1024 * 1024


def dot_t(a, b):
    return lax.dot_general(a, b, (((1,), (1,)), ((), ())), preferred_element_type=F32)


def dot_n(a, b):
    return lax.dot_general(a, b, (((1,), (0,)), ((), ())), preferred_element_type=F32)


def in_hbm(x):
    return pltpu.with_memory_space_constraint(x, pltpu.HBM)


def left_half(rows, lanes):
    return lax.broadcasted_iota(jnp.int32, (rows, lanes), 1) < lanes // 2


def swap_halves(tile):
    half = tile.shape[1] // 2
    return jnp.concatenate([tile[:, half:], tile[:, :half]], axis=1)


def beside(tiles, mask):
    tops, bots = [], []
    for a, b in zip(tiles[::2], tiles[1::2]):
        tops.append(jnp.where(mask, a, swap_halves(b)))
        bots.append(jnp.where(mask, swap_halves(a), b))
    return jnp.concatenate([jnp.concatenate(tops, axis=1), jnp.concatenate(bots, axis=1)], axis=0)


def dense(pair, mask):
    half = pair.shape[0] // 2
    top, bot = pair[:half], pair[half:]
    return jnp.where(mask, top, swap_halves(bot)), jnp.where(mask, swap_halves(top), bot)


def diagonal(a, b):
    zero = jnp.zeros_like(a)
    return jnp.concatenate(
        [jnp.concatenate([a, zero], axis=1), jnp.concatenate([zero, b], axis=1)], axis=0
    )


def upward_kernel(
    me_ref, pts_hbm, basis_hbm, trans_hbm, owner_hbm, local_hbm, coeff_ref, pay_ref, side_ref, place_ref,
    pts_ref, basis_ref, trans_ref, owner_ref, local_ref, sems, place_sems, *, steps
):
    leaves, n, _ = pts_ref.shape
    parents = trans_ref.shape[0]
    mask = left_half(n // 2, 128)
    pairs = parents // steps

    def copies(i):
        own = pl.ds(i * pairs, pairs)
        both = pl.ds(2 * i * pairs, 2 * pairs)
        return (
            pltpu.make_async_copy(pts_hbm.at[both], pts_ref.at[both], sems.at[0, i]),
            pltpu.make_async_copy(basis_hbm.at[both], basis_ref.at[both], sems.at[1, i]),
            pltpu.make_async_copy(trans_hbm.at[own], trans_ref.at[own], sems.at[2, i]),
        )

    for i in range(steps):
        for c in copies(i):
            c.start(priority=min(i, 1))
    listed = (
        pltpu.make_async_copy(owner_hbm, owner_ref, place_sems.at[0]),
        pltpu.make_async_copy(local_hbm, local_ref, place_sems.at[1]),
    )
    for c in listed:
        c.start(priority=1)

    for i in range(steps):
        for c in copies(i):
            c.wait()
        own = range(i * pairs, (i + 1) * pairs)
        paired = []
        for p in own:
            x = jnp.concatenate([pts_ref[2 * p], pts_ref[2 * p + 1]], axis=1)
            paired.append(dot_t(x, diagonal(basis_ref[2 * p], basis_ref[2 * p + 1])).astype(BF16))
        ups = []
        for q in range(0, pairs, 2):
            x = jnp.concatenate([paired[q], paired[q + 1]], axis=1)
            ups.append(dot_t(x, diagonal(trans_ref[own[q]], trans_ref[own[q + 1]])).astype(BF16))
        for q, p in enumerate(own):
            coeff_ref[2 * p], coeff_ref[2 * p + 1] = dense(paired[q], mask)
        for q, up in enumerate(ups):
            p = own[2 * q]
            pay_ref[p], pay_ref[p + 1] = dense(up, mask)

    def edge(ref, at, first):
        lo = 0 if first else leaves - FAR
        for q in range(FAR):
            ref[at + q] = coeff_ref[lo + q]
        lo = 0 if first else leaves - NEAR
        for q in range(NEAR):
            x = pts_ref[lo + q]
            ref[at + FAR + 2 * q] = x[: n // 2]
            ref[at + FAR + 2 * q + 1] = x[n // 2 :]

    odd = me_ref[0] & 1 == 1

    @pl.when(odd)
    def _():
        edge(pay_ref, parents, True)
        edge(side_ref, 0, False)

    @pl.when(jnp.logical_not(odd))
    def _():
        edge(side_ref, 0, True)
        edge(pay_ref, parents, False)

    for c in listed:
        c.wait()
    place_ref[...] = (owner_ref[...] ^ me_ref[0]) * parents + local_ref[...]


def upward(me, points, basis, transfer, owner, local):
    leaves, n, _ = points.shape
    parents, rank, _ = transfer.shape
    steps = 2
    halo = FAR + 2 * NEAR
    tile = (n // 2, 2 * rank)
    smem = pl.BlockSpec(memory_space=pltpu.SMEM)
    vmem = pl.BlockSpec(memory_space=pltpu.VMEM)
    hbm = pl.BlockSpec(memory_space=pltpu.HBM)
    return pl.pallas_call(
        functools.partial(upward_kernel, steps=steps),
        out_shape=(
            jax.ShapeDtypeStruct((leaves,) + tile, BF16),
            jax.ShapeDtypeStruct((parents + halo,) + tile, BF16),
            jax.ShapeDtypeStruct((halo,) + tile, BF16),
            jax.ShapeDtypeStruct(owner.shape, jnp.int32),
        ),
        in_specs=[smem] + [hbm] * 5,
        out_specs=[vmem] * 4,
        scratch_shapes=[
            pltpu.VMEM(points.shape, BF16),
            pltpu.VMEM(basis.shape, BF16),
            pltpu.VMEM(transfer.shape, BF16),
            pltpu.VMEM(owner.shape, jnp.int32),
            pltpu.VMEM(owner.shape, jnp.int32),
            pltpu.SemaphoreType.DMA((3, steps)),
            pltpu.SemaphoreType.DMA((2,)),
        ],
        compiler_params=pltpu.CompilerParams(vmem_limit_bytes=LIMIT),
        name="upward",
    )(me, *[in_hbm(x) for x in (points, basis, transfer, owner, local)])


def local_kernel(
    me_ref, noff_hbm, coff_hbm, pts_hbm, near_hbm, coup_hbm, coeff_ref, *refs, leafs, base, stride, edges
):
    if edges:
        pay_ref, side_ref, hop_ref, *refs = refs
    near_out, field_out, noff_ref, coff_ref, pts_pad, coeff_pad, near_ref, coup_ref, sems, first_sems = refs
    leaves, n, _ = pts_hbm.shape
    steps, chunk, slots = near_ref.shape[:3]
    far_slots = coff_ref.shape[0]
    mask = left_half(n // 2, 128)

    def copies(i):
        own = pl.ds(base + stride * i, chunk)
        return (
            pltpu.make_async_copy(near_hbm.at[own], near_ref.at[i], sems.at[0, i]),
            pltpu.make_async_copy(coup_hbm.at[own], coup_ref.at[i], sems.at[1, i]),
        )

    early = (
        pltpu.make_async_copy(noff_hbm, noff_ref, first_sems.at[0]),
        pltpu.make_async_copy(coff_hbm, coff_ref, first_sems.at[1]),
        pltpu.make_async_copy(pts_hbm, pts_pad.at[pl.ds(NEAR, leaves)], first_sems.at[2]),
    )
    for c in early:
        c.start()
    for i in range(min(AHEAD, steps)):
        for c in copies(i):
            c.start()

    coeff_pad[FAR : FAR + leaves] = coeff_ref[...]

    def put(ref, at, low):
        co = 0 if low else leaves + FAR
        po = 0 if low else leaves + NEAR
        for q in range(FAR):
            coeff_pad[co + q] = ref[at + q]
        for q in range(NEAR):
            pts_pad[po + q, : n // 2] = ref[at + FAR + 2 * q]
            pts_pad[po + q, n // 2 :] = ref[at + FAR + 2 * q + 1]

    if edges:
        at = pay_ref.shape[0] - side_ref.shape[0]
        leaf = me_ref[0] & (leafs - 1)
        odd = leaf & 1 == 1

        def put_side(low):
            last = leaf == (0 if low else leafs - 1)

            @pl.when(last)
            def _():
                put(hop_ref, 0, low)

            @pl.when(jnp.logical_not(last))
            def _():
                put(side_ref, 0, low)

        @pl.when(odd)
        def _():
            put(pay_ref, at, True)
            put_side(False)

        @pl.when(jnp.logical_not(odd))
        def _():
            put_side(True)
            put(pay_ref, at, False)

    for c in early:
        c.wait()

    def body(i, carry):
        for c in copies(i):
            c.wait()

        @pl.when(i + AHEAD < steps)
        def _():
            for c in copies(i + AHEAD):
                c.start()

        nears, fields = [], []
        for j in range(chunk):
            c = base + stride * i + j
            xs = [pts_pad[c + NEAR + noff_ref[k, c]] for k in range(slots)]
            ws = [near_ref[i, j, k] for k in range(slots)]
            nears.append(dot_t(jnp.concatenate(xs, axis=1), jnp.concatenate(ws, axis=1)))
        for j in range(chunk):
            c = base + stride * i + j
            lhs = beside([coeff_pad[c + FAR + coff_ref[k, c]] for k in range(far_slots)], mask)
            fields.append(dot_t(lhs, coup_ref[i, j]))
        for j in range(chunk):
            near_out[i * chunk + j] = nears[j]
        for j in range(0, chunk, 2):
            field_out[(i * chunk + j) // 2] = jnp.concatenate([fields[j], fields[j + 1]], axis=1)
        return carry

    lax.fori_loop(0, steps, body, 0)


def local_terms(
    me, near_offsets, coupling_offsets, points, coeffs, halos, near_blocks, leaf_coupling, leafs, base, stride, steps, chunk
):
    leaves, n, size = points.shape
    rank = leaf_coupling.shape[1]
    tile = coeffs.shape[1:]
    smem = pl.BlockSpec(memory_space=pltpu.SMEM)
    vmem = pl.BlockSpec(memory_space=pltpu.VMEM)
    hbm = pl.BlockSpec(memory_space=pltpu.HBM)
    return pl.pallas_call(
        functools.partial(local_kernel, leafs=leafs, base=base, stride=stride, edges=bool(halos)),
        out_shape=(
            jax.ShapeDtypeStruct((steps * chunk, n, size), F32),
            jax.ShapeDtypeStruct((steps * chunk // 2, n, 2 * rank), F32),
        ),
        in_specs=[smem] + [hbm] * 5 + [vmem] * (1 + len(halos)),
        out_specs=[vmem] * 2,
        scratch_shapes=[
            pltpu.SMEM(near_offsets.shape, jnp.int32),
            pltpu.SMEM(coupling_offsets.shape, jnp.int32),
            pltpu.VMEM((leaves + 2 * NEAR, n, size), BF16),
            pltpu.VMEM((leaves + 2 * FAR,) + tile, BF16),
            pltpu.VMEM((steps, chunk) + near_blocks.shape[1:], BF16),
            pltpu.VMEM((steps, chunk) + leaf_coupling.shape[1:], BF16),
            pltpu.SemaphoreType.DMA((2, steps)),
            pltpu.SemaphoreType.DMA((3,)),
        ],
        compiler_params=pltpu.CompilerParams(vmem_limit_bytes=LIMIT),
        name="local_terms",
    )(
        me, *[in_hbm(x) for x in (near_offsets, coupling_offsets, points, near_blocks, leaf_coupling)],
        coeffs, *halos,
    )


def downward_kernel(
    place_hbm, table, coup_ref, trans_ref, basis_ref, near_mid, field_mid, near_rim, field_rim, out_hbm,
    place_ref, out_ref, sems, place_sem, *, batch
):
    parents = trans_ref.shape[0]
    n, size = near_mid.shape[1:]
    slots = place_ref.shape[0]
    mask = left_half(n // 2, 128)
    rim = field_rim.shape[0] // 2
    fetch = pltpu.make_async_copy(place_hbm, place_ref, place_sem)
    fetch.start()
    fetch.wait()

    def run(own, near_ref, field_ref, at):
        halves = []
        for p in own:
            tiles = [table[place_ref[k, p]] for k in range(slots)]
            halves.append(dot_t(beside(tiles, mask), coup_ref[p]).astype(BF16))
        totals = []
        for q, (p, half) in enumerate(zip(own, halves)):
            totals.append((field_ref[at + q] + dot_n(half, trans_ref[p])).astype(BF16))
        fars = []
        for p, total in zip(own, totals):
            fars.append(dot_n(total, diagonal(basis_ref[2 * p], basis_ref[2 * p + 1])))
        for q, (p, far) in enumerate(zip(own, fars)):
            out_ref[2 * p] = (far[:, :size] + near_ref[2 * (at + q)]).astype(BF16)
            out_ref[2 * p + 1] = (far[:, size:] + near_ref[2 * (at + q) + 1]).astype(BF16)

    def copy(first, count, sem):
        own = pl.ds(2 * first, 2 * count)
        return pltpu.make_async_copy(out_ref.at[own], out_hbm.at[own], sem)

    def rows(step, carry):
        first = rim + step * batch
        run([first + q for q in range(batch)], near_mid, field_mid, step * batch)
        copy(first, batch, sems.at[step]).start()
        return carry

    steps = (parents - 2 * rim) // batch
    lax.fori_loop(0, steps, rows, 0)
    run(list(range(rim)) + list(range(parents - rim, parents)), near_rim, field_rim, 0)
    ends = [copy(0, rim, sems.at[steps]), copy(parents - rim, rim, sems.at[steps + 1])]
    for c in ends:
        c.start()
    for step in range(steps):
        copy(rim + step * batch, batch, sems.at[step]).wait()
    for c in ends:
        c.wait()


def downward(place, table, coupling, transfer, basis, mid, rim):
    leaves, _, size = basis.shape
    n = mid[0].shape[1]
    vmem = pl.BlockSpec(memory_space=pltpu.VMEM)
    big = [pltpu.with_memory_space_constraint(x, pltpu.VMEM) for x in (table, coupling, transfer, basis, *mid, *rim)]
    batch = mid[1].shape[0] // 2
    return pl.pallas_call(
        functools.partial(downward_kernel, batch=batch),
        out_shape=jax.ShapeDtypeStruct((leaves, n, size), BF16),
        in_specs=[pl.BlockSpec(memory_space=pl.ANY)] + [vmem] * len(big),
        out_specs=pl.BlockSpec(memory_space=pltpu.HBM),
        scratch_shapes=[
            pltpu.SMEM(place.shape, jnp.int32),
            pltpu.VMEM((leaves, n, size), BF16),
            pltpu.SemaphoreType.DMA((4,)),
            pltpu.SemaphoreType.DMA,
        ],
        compiler_params=pltpu.CompilerParams(vmem_limit_bytes=LIMIT),
        name="downward",
    )(place, *big)


def on_device(
    points_rhs,
    leaf_basis,
    transfer,
    leaf_coupling,
    parent_coupling,
    near_blocks,
    near_offsets,
    coupling_offsets,
    parent_owner,
    parent_local,
):
    streams, leafs = lax.axis_size("stream"), lax.axis_size("leaf")
    devices = streams * leafs
    parents = transfer.shape[0]
    me = lax.axis_index(AXES).astype(jnp.int32)
    flag = me.reshape(1)

    my_leaf = me % leafs

    def permute(x, pairs):
        return lax.ppermute(x, AXES, pairs)

    def swap(x, bits):
        return permute(x, [(i, i ^ bits) for i in range(devices)])

    coeffs, payload, side, place = upward(flag, points_rhs, leaf_basis, transfer, parent_owner.T, parent_local.T)

    got = swap(payload, 1)
    line = [payload[:parents], got[:parents]]
    sides = None
    for k in range(2, leafs):
        if k & (k + 1):
            line.append(swap(line[0], k))
            continue
        both = swap(jnp.concatenate([line[0], side], axis=0), k)
        line.append(both[:parents])
        if sides is None:
            sides = both[parents:]
        else:
            away = my_leaf ^ jnp.where(my_leaf % 2 == 1, my_leaf + 1, my_leaf - 1)
            sides = jnp.where((away == k) | (k == leafs - 1) & (away > k) | (away < 0), both[parents:], sides)
    ends = [(s * leafs, (s + 1) * leafs) for s in range(streams - 1)]
    ends += [(s * leafs + leafs - 1, s * leafs - 1) for s in range(1, streams)]
    hop = permute(sides, ends)

    def join(parts):
        return parts[0] if len(parts) == 1 else jnp.concatenate(parts, axis=0)

    groups = [(0, [join(line[:2])]), (2, [join(line[2:])])]
    pieces = {}
    for base, parts in groups:
        have = {0: parts}
        for s in range(2, streams, 2):
            low = s & -s
            high = 1 << (s.bit_length() - 1)
            if low == high:
                have[s] = [swap(x, s * leafs) for x in have[s ^ low]]
                continue
            near, far = have[s ^ low], have[s ^ high]
            if len(near) == 1:
                rows = near[0].shape[0] // 2
                near, far = (near[0][:rows], None), (None, far[0][rows:])
            have[s] = [swap(far[j], high * leafs) if j % 2 else swap(near[j], low * leafs) for j in range(len(near))]
        for s in list(have):
            have[s] = join(have[s])
            have[s ^ 1] = swap(have[s], leafs)
        for s, g in have.items():
            pieces[s * leafs + base] = g
    table = jnp.concatenate([pieces[k] for k in sorted(pieces)], axis=0)

    leaves = points_rhs.shape[0]
    rim = 8
    chunk = (leaves - 2 * rim) // 3
    args = (flag, near_offsets.T, coupling_offsets.T, points_rhs, coeffs)
    mid = local_terms(*args, (), near_blocks, leaf_coupling, leafs, rim, chunk, 3, chunk)
    edge = local_terms(*args, (got, sides, hop), near_blocks, leaf_coupling, leafs, 0, leaves - rim, 2, rim)
    return downward(place, table, parent_coupling, transfer, leaf_basis, mid, edge)


def solution(mesh):
    three = P(AXES, None, None)
    two = P(AXES, None)
    return jax.shard_map(
        on_device,
        mesh=mesh,
        in_specs=(three,) * 5 + (P(AXES, None, None, None),) + (two,) * 4,
        out_specs=three,
        check_vma=False,
    )
```

```python
import functools

import jax
import jax.numpy as jnp
from jax import lax
from jax.experimental import pallas as pl
from jax.experimental.pallas import tpu as pltpu
from jax.sharding import PartitionSpec as P


AXES = ("stream", "leaf")
FAR = 5
NEAR = 2
F32 = jnp.float32
BF16 = jnp.bfloat16

AHEAD = 2
LIMIT = 16 * 1024 * 1024


def dot_t(a, b):
    return lax.dot_general(a, b, (((1,), (1,)), ((), ())), preferred_element_type=F32)


def dot_n(a, b):
    return lax.dot_general(a, b, (((1,), (0,)), ((), ())), preferred_element_type=F32)


def in_hbm(x):
    return pltpu.with_memory_space_constraint(x, pltpu.HBM)


def left_half(rows, lanes):
    return lax.broadcasted_iota(jnp.int32, (rows, lanes), 1) < lanes // 2


def swap_halves(tile):
    half = tile.shape[1] // 2
    return jnp.concatenate([tile[:, half:], tile[:, :half]], axis=1)


def beside(tiles, mask):
    tops, bots = [], []
    for a, b in zip(tiles[::2], tiles[1::2]):
        tops.append(jnp.where(mask, a, swap_halves(b)))
        bots.append(jnp.where(mask, swap_halves(a), b))
    return jnp.concatenate([jnp.concatenate(tops, axis=1), jnp.concatenate(bots, axis=1)], axis=0)


def dense(pair, mask):
    half = pair.shape[0] // 2
    top, bot = pair[:half], pair[half:]
    return jnp.where(mask, top, swap_halves(bot)), jnp.where(mask, swap_halves(top), bot)


def diagonal(a, b):
    zero = jnp.zeros_like(a)
    return jnp.concatenate(
        [jnp.concatenate([a, zero], axis=1), jnp.concatenate([zero, b], axis=1)], axis=0
    )


def upward_kernel(
    me_ref, pts_hbm, basis_hbm, trans_hbm, owner_hbm, local_hbm, coeff_ref, pay_ref, edge_ref, side_ref, place_ref,
    pts_ref, basis_ref, trans_ref, owner_ref, local_ref, sems, place_sems, *, steps
):
    leaves, n, _ = pts_ref.shape
    parents = trans_ref.shape[0]
    mask = left_half(n // 2, 128)
    pairs = parents // steps

    def copies(i):
        own = pl.ds(i * pairs, pairs)
        both = pl.ds(2 * i * pairs, 2 * pairs)
        return (
            pltpu.make_async_copy(pts_hbm.at[both], pts_ref.at[both], sems.at[0, i]),
            pltpu.make_async_copy(basis_hbm.at[both], basis_ref.at[both], sems.at[1, i]),
            pltpu.make_async_copy(trans_hbm.at[own], trans_ref.at[own], sems.at[2, i]),
        )

    for i in range(steps):
        for c in copies(i):
            c.start(priority=min(i, 1))
    listed = (
        pltpu.make_async_copy(owner_hbm, owner_ref, place_sems.at[0]),
        pltpu.make_async_copy(local_hbm, local_ref, place_sems.at[1]),
    )
    for c in listed:
        c.start(priority=1)

    for i in range(steps):
        for c in copies(i):
            c.wait()
        own = range(i * pairs, (i + 1) * pairs)
        paired = []
        for p in own:
            x = jnp.concatenate([pts_ref[2 * p], pts_ref[2 * p + 1]], axis=1)
            paired.append(dot_t(x, diagonal(basis_ref[2 * p], basis_ref[2 * p + 1])).astype(BF16))
        ups = []
        for q in range(0, pairs, 2):
            x = jnp.concatenate([paired[q], paired[q + 1]], axis=1)
            ups.append(dot_t(x, diagonal(trans_ref[own[q]], trans_ref[own[q + 1]])).astype(BF16))
        for q, p in enumerate(own):
            coeff_ref[2 * p], coeff_ref[2 * p + 1] = dense(paired[q], mask)
        for q, up in enumerate(ups):
            p = own[2 * q]
            pay_ref[p], pay_ref[p + 1] = dense(up, mask)

    def edge(ref, first):
        lo = 0 if first else leaves - FAR
        for q in range(FAR):
            ref[q] = coeff_ref[lo + q]
        lo = 0 if first else leaves - NEAR
        for q in range(NEAR):
            x = pts_ref[lo + q]
            ref[FAR + 2 * q] = x[: n // 2]
            ref[FAR + 2 * q + 1] = x[n // 2 :]

    odd = me_ref[0] & 1 == 1

    @pl.when(odd)
    def _():
        edge(edge_ref, True)
        edge(side_ref, False)

    @pl.when(jnp.logical_not(odd))
    def _():
        edge(side_ref, True)
        edge(edge_ref, False)

    for c in listed:
        c.wait()
    place_ref[...] = (owner_ref[...] ^ me_ref[0]) * parents + local_ref[...]


def upward(me, points, basis, transfer, owner, local):
    leaves, n, _ = points.shape
    parents, rank, _ = transfer.shape
    steps = 2
    halo = FAR + 2 * NEAR
    tile = (n // 2, 2 * rank)
    smem = pl.BlockSpec(memory_space=pltpu.SMEM)
    vmem = pl.BlockSpec(memory_space=pltpu.VMEM)
    hbm = pl.BlockSpec(memory_space=pltpu.HBM)
    return pl.pallas_call(
        functools.partial(upward_kernel, steps=steps),
        out_shape=(
            jax.ShapeDtypeStruct((leaves,) + tile, BF16),
            jax.ShapeDtypeStruct((parents,) + tile, BF16),
            jax.ShapeDtypeStruct((halo,) + tile, BF16),
            jax.ShapeDtypeStruct((halo,) + tile, BF16),
            jax.ShapeDtypeStruct(owner.shape, jnp.int32),
        ),
        in_specs=[smem] + [hbm] * 5,
        out_specs=[vmem] * 5,
        scratch_shapes=[
            pltpu.VMEM(points.shape, BF16),
            pltpu.VMEM(basis.shape, BF16),
            pltpu.VMEM(transfer.shape, BF16),
            pltpu.VMEM(owner.shape, jnp.int32),
            pltpu.VMEM(owner.shape, jnp.int32),
            pltpu.SemaphoreType.DMA((3, steps)),
            pltpu.SemaphoreType.DMA((2,)),
        ],
        compiler_params=pltpu.CompilerParams(vmem_limit_bytes=LIMIT),
        name="upward",
    )(me, *[in_hbm(x) for x in (points, basis, transfer, owner, local)])


def local_kernel(
    me_ref, noff_hbm, coff_hbm, pts_hbm, near_hbm, coup_hbm, coeff_ref, *refs, leafs, base, stride, edges
):
    if edges:
        edge_ref, side_ref, hop_ref, *refs = refs
    near_out, field_out, noff_ref, coff_ref, pts_pad, coeff_pad, near_ref, coup_ref, sems, first_sems = refs
    leaves, n, _ = pts_hbm.shape
    steps, chunk, slots = near_ref.shape[:3]
    far_slots = coff_ref.shape[0]
    mask = left_half(n // 2, 128)

    def copies(i):
        own = pl.ds(base + stride * i, chunk)
        return (
            pltpu.make_async_copy(near_hbm.at[own], near_ref.at[i], sems.at[0, i]),
            pltpu.make_async_copy(coup_hbm.at[own], coup_ref.at[i], sems.at[1, i]),
        )

    early = (
        pltpu.make_async_copy(noff_hbm, noff_ref, first_sems.at[0]),
        pltpu.make_async_copy(coff_hbm, coff_ref, first_sems.at[1]),
        pltpu.make_async_copy(pts_hbm, pts_pad.at[pl.ds(NEAR, leaves)], first_sems.at[2]),
    )
    for c in early:
        c.start()
    for i in range(min(AHEAD, steps)):
        for c in copies(i):
            c.start()

    coeff_pad[FAR : FAR + leaves] = coeff_ref[...]

    def put(ref, low):
        co = 0 if low else leaves + FAR
        po = 0 if low else leaves + NEAR
        for q in range(FAR):
            coeff_pad[co + q] = ref[q]
        for q in range(NEAR):
            pts_pad[po + q, : n // 2] = ref[FAR + 2 * q]
            pts_pad[po + q, n // 2 :] = ref[FAR + 2 * q + 1]

    if edges:
        leaf = me_ref[0] & (leafs - 1)
        odd = leaf & 1 == 1

        def put_side(low):
            last = leaf == (0 if low else leafs - 1)

            @pl.when(last)
            def _():
                put(hop_ref, low)

            @pl.when(jnp.logical_not(last))
            def _():
                put(side_ref, low)

        @pl.when(odd)
        def _():
            put(edge_ref, True)
            put_side(False)

        @pl.when(jnp.logical_not(odd))
        def _():
            put_side(True)
            put(edge_ref, False)

    for c in early:
        c.wait()

    def body(i, carry):
        for c in copies(i):
            c.wait()

        @pl.when(i + AHEAD < steps)
        def _():
            for c in copies(i + AHEAD):
                c.start()

        nears, fields = [], []
        for j in range(chunk):
            c = base + stride * i + j
            xs = [pts_pad[c + NEAR + noff_ref[k, c]] for k in range(slots)]
            ws = [near_ref[i, j, k] for k in range(slots)]
            nears.append(dot_t(jnp.concatenate(xs, axis=1), jnp.concatenate(ws, axis=1)))
        for j in range(chunk):
            c = base + stride * i + j
            lhs = beside([coeff_pad[c + FAR + coff_ref[k, c]] for k in range(far_slots)], mask)
            fields.append(dot_t(lhs, coup_ref[i, j]))
        for j in range(chunk):
            near_out[i * chunk + j] = nears[j]
        for j in range(0, chunk, 2):
            field_out[(i * chunk + j) // 2] = jnp.concatenate([fields[j], fields[j + 1]], axis=1)
        return carry

    lax.fori_loop(0, steps, body, 0)


def local_terms(
    me, near_offsets, coupling_offsets, points, coeffs, halos, near_blocks, leaf_coupling, leafs, base, stride, steps, chunk
):
    leaves, n, size = points.shape
    rank = leaf_coupling.shape[1]
    tile = coeffs.shape[1:]
    smem = pl.BlockSpec(memory_space=pltpu.SMEM)
    vmem = pl.BlockSpec(memory_space=pltpu.VMEM)
    hbm = pl.BlockSpec(memory_space=pltpu.HBM)
    return pl.pallas_call(
        functools.partial(local_kernel, leafs=leafs, base=base, stride=stride, edges=bool(halos)),
        out_shape=(
            jax.ShapeDtypeStruct((steps * chunk, n, size), F32),
            jax.ShapeDtypeStruct((steps * chunk // 2, n, 2 * rank), F32),
        ),
        in_specs=[smem] + [hbm] * 5 + [vmem] * (1 + len(halos)),
        out_specs=[vmem] * 2,
        scratch_shapes=[
            pltpu.SMEM(near_offsets.shape, jnp.int32),
            pltpu.SMEM(coupling_offsets.shape, jnp.int32),
            pltpu.VMEM((leaves + 2 * NEAR, n, size), BF16),
            pltpu.VMEM((leaves + 2 * FAR,) + tile, BF16),
            pltpu.VMEM((steps, chunk) + near_blocks.shape[1:], BF16),
            pltpu.VMEM((steps, chunk) + leaf_coupling.shape[1:], BF16),
            pltpu.SemaphoreType.DMA((2, steps)),
            pltpu.SemaphoreType.DMA((3,)),
        ],
        compiler_params=pltpu.CompilerParams(vmem_limit_bytes=LIMIT),
        name="local_terms",
    )(
        me, *[in_hbm(x) for x in (near_offsets, coupling_offsets, points, near_blocks, leaf_coupling)],
        coeffs, *halos,
    )


def downward_kernel(
    place_hbm, table, coup_ref, trans_ref, basis_ref, near_mid, field_mid, near_rim, field_rim, out_hbm,
    place_ref, half_ref, total_ref, out_ref, sems, place_sem, *, batch
):
    parents = trans_ref.shape[0]
    n, size = near_mid.shape[1:]
    slots = place_ref.shape[0]
    mask = left_half(n // 2, 128)
    rim = field_rim.shape[0] // 2
    fetch = pltpu.make_async_copy(place_hbm, place_ref, place_sem)
    fetch.start()
    fetch.wait()

    def local_at(p):
        if rim <= p < parents - rim:
            return near_mid, field_mid, p - rim
        return near_rim, field_rim, p if p < rim else p - parents + 2 * rim

    def copy(step):
        own = pl.ds(2 * step * batch, 2 * batch)
        return pltpu.make_async_copy(out_ref.at[own], out_hbm.at[own], sems.at[step])

    for p in range(parents):
        tiles = [table[place_ref[k, p]] for k in range(slots)]
        half_ref[p] = dot_t(beside(tiles, mask), coup_ref[p]).astype(BF16)
    for p in range(parents):
        _, field_ref, at = local_at(p)
        total_ref[p] = (field_ref[at] + dot_n(half_ref[p], trans_ref[p])).astype(BF16)
    for step in range(parents // batch):
        for p in range(step * batch, (step + 1) * batch):
            near_ref, _, at = local_at(p)
            far = dot_n(total_ref[p], diagonal(basis_ref[2 * p], basis_ref[2 * p + 1]))
            out_ref[2 * p] = (far[:, :size] + near_ref[2 * at]).astype(BF16)
            out_ref[2 * p + 1] = (far[:, size:] + near_ref[2 * at + 1]).astype(BF16)
        copy(step).start()
    for step in range(parents // batch):
        copy(step).wait()


def downward(place, table, coupling, transfer, basis, mid, rim):
    leaves, _, size = basis.shape
    n = mid[0].shape[1]
    vmem = pl.BlockSpec(memory_space=pltpu.VMEM)
    big = [pltpu.with_memory_space_constraint(x, pltpu.VMEM) for x in (table, coupling, transfer, basis, *mid, *rim)]
    parents, rank, _ = transfer.shape
    batch = parents // 4
    return pl.pallas_call(
        functools.partial(downward_kernel, batch=batch),
        out_shape=jax.ShapeDtypeStruct((leaves, n, size), BF16),
        in_specs=[pl.BlockSpec(memory_space=pl.ANY)] + [vmem] * len(big),
        out_specs=pl.BlockSpec(memory_space=pltpu.HBM),
        scratch_shapes=[
            pltpu.SMEM(place.shape, jnp.int32),
            pltpu.VMEM((parents, n, rank), BF16),
            pltpu.VMEM((parents, n, 2 * rank), BF16),
            pltpu.VMEM((leaves, n, size), BF16),
            pltpu.SemaphoreType.DMA((parents // batch,)),
            pltpu.SemaphoreType.DMA,
        ],
        compiler_params=pltpu.CompilerParams(vmem_limit_bytes=LIMIT),
        name="downward",
    )(place, *big)


def on_device(
    points_rhs,
    leaf_basis,
    transfer,
    leaf_coupling,
    parent_coupling,
    near_blocks,
    near_offsets,
    coupling_offsets,
    parent_owner,
    parent_local,
):
    streams, leafs = lax.axis_size("stream"), lax.axis_size("leaf")
    devices = streams * leafs
    me = lax.axis_index(AXES).astype(jnp.int32)
    flag = me.reshape(1)

    my_leaf = me % leafs

    def permute(x, pairs):
        return lax.ppermute(x, AXES, pairs)

    def swap(x, bits):
        return permute(x, [(i, i ^ bits) for i in range(devices)])

    coeffs, own, edge, side, place = upward(flag, points_rhs, leaf_basis, transfer, parent_owner.T, parent_local.T)

    line = [own] + [swap(own, k) for k in range(1, leafs)]
    edges = swap(edge, 1)
    sides, k = None, 3
    while k < leafs:
        both = swap(side, k)
        if sides is None:
            sides = both
        else:
            away = my_leaf ^ jnp.where(my_leaf % 2 == 1, my_leaf + 1, my_leaf - 1)
            sides = jnp.where((away == k) | (k == leafs - 1) & (away > k) | (away < 0), both, sides)
        k = 2 * k + 1
    ends = [(s * leafs, (s + 1) * leafs) for s in range(streams - 1)]
    ends += [(s * leafs + leafs - 1, s * leafs - 1) for s in range(1, streams)]
    hop = permute(sides, ends)

    def join(parts):
        return parts[0] if len(parts) == 1 else jnp.concatenate(parts, axis=0)

    groups = [(0, [join(line[:2])]), (2, [join(line[2:])])]
    pieces = {}
    for base, parts in groups:
        have = {0: parts}
        for s in range(2, streams, 2):
            low = s & -s
            high = 1 << (s.bit_length() - 1)
            if low == high:
                have[s] = [swap(x, s * leafs) for x in have[s ^ low]]
                continue
            near, far = have[s ^ low], have[s ^ high]
            if len(near) == 1:
                rows = near[0].shape[0] // 2
                near, far = (near[0][:rows], None), (None, far[0][rows:])
            have[s] = [swap(far[j], high * leafs) if j % 2 else swap(near[j], low * leafs) for j in range(len(near))]
        for s in list(have):
            have[s] = join(have[s])
            have[s ^ 1] = swap(have[s], leafs)
        for s, g in have.items():
            pieces[s * leafs + base] = g
    table = jnp.concatenate([pieces[k] for k in sorted(pieces)], axis=0)

    leaves = points_rhs.shape[0]
    rim = 8
    chunk = (leaves - 2 * rim) // 3
    args = (flag, near_offsets.T, coupling_offsets.T, points_rhs, coeffs)
    mid = local_terms(*args, (), near_blocks, leaf_coupling, leafs, rim, chunk, 3, chunk)
    edge = local_terms(*args, (edges, sides, hop), near_blocks, leaf_coupling, leafs, 0, leaves - rim, 2, rim)
    return downward(place, table, parent_coupling, transfer, leaf_basis, mid, edge)


def solution(mesh):
    three = P(AXES, None, None)
    two = P(AXES, None)
    return jax.shard_map(
        on_device,
        mesh=mesh,
        in_specs=(three,) * 5 + (P(AXES, None, None, None),) + (two,) * 4,
        out_specs=three,
        check_vma=False,
    )
```

```python
import functools

import jax
import jax.numpy as jnp
from jax import lax
from jax.experimental import pallas as pl
from jax.experimental.pallas import tpu as pltpu
from jax.sharding import PartitionSpec as P


AXES = ("stream", "leaf")
FAR = 5
NEAR = 2
F32 = jnp.float32
BF16 = jnp.bfloat16

AHEAD = 3
LIMIT = 16 * 1024 * 1024


def dot_t(a, b):
    return lax.dot_general(a, b, (((1,), (1,)), ((), ())), preferred_element_type=F32)


def dot_n(a, b):
    return lax.dot_general(a, b, (((1,), (0,)), ((), ())), preferred_element_type=F32)


def in_hbm(x):
    return pltpu.with_memory_space_constraint(x, pltpu.HBM)


def left_half(rows, lanes):
    return lax.broadcasted_iota(jnp.int32, (rows, lanes), 1) < lanes // 2


def swap_halves(tile):
    half = tile.shape[1] // 2
    return jnp.concatenate([tile[:, half:], tile[:, :half]], axis=1)


def beside(tiles, mask):
    tops, bots = [], []
    for a, b in zip(tiles[::2], tiles[1::2]):
        tops.append(jnp.where(mask, a, swap_halves(b)))
        bots.append(jnp.where(mask, swap_halves(a), b))
    return jnp.concatenate([jnp.concatenate(tops, axis=1), jnp.concatenate(bots, axis=1)], axis=0)


def dense(pair, mask):
    half = pair.shape[0] // 2
    top, bot = pair[:half], pair[half:]
    return jnp.where(mask, top, swap_halves(bot)), jnp.where(mask, swap_halves(top), bot)


def diagonal(a, b):
    zero = jnp.zeros_like(a)
    return jnp.concatenate(
        [jnp.concatenate([a, zero], axis=1), jnp.concatenate([zero, b], axis=1)], axis=0
    )


def upward_kernel(
    me_ref, pts_hbm, basis_hbm, trans_hbm, owner_hbm, local_hbm, coeff_ref, pay_ref, edge_ref, side_ref, place_ref,
    pts_ref, basis_ref, trans_ref, owner_ref, local_ref, sems, place_sems, *, steps
):
    leaves, n, _ = pts_ref.shape
    parents = trans_ref.shape[0]
    mask = left_half(n // 2, 128)
    pairs = parents // steps

    def copies(i):
        own = pl.ds(i * pairs, pairs)
        both = pl.ds(2 * i * pairs, 2 * pairs)
        return (
            pltpu.make_async_copy(pts_hbm.at[both], pts_ref.at[both], sems.at[0, i]),
            pltpu.make_async_copy(basis_hbm.at[both], basis_ref.at[both], sems.at[1, i]),
            pltpu.make_async_copy(trans_hbm.at[own], trans_ref.at[own], sems.at[2, i]),
        )

    for i in range(steps):
        for c in copies(i):
            c.start(priority=min(i, 1))
    listed = (
        pltpu.make_async_copy(owner_hbm, owner_ref, place_sems.at[0]),
        pltpu.make_async_copy(local_hbm, local_ref, place_sems.at[1]),
    )
    for c in listed:
        c.start(priority=1)

    for i in range(steps):
        for c in copies(i):
            c.wait()
        own = range(i * pairs, (i + 1) * pairs)
        paired = []
        for p in own:
            x = jnp.concatenate([pts_ref[2 * p], pts_ref[2 * p + 1]], axis=1)
            paired.append(dot_t(x, diagonal(basis_ref[2 * p], basis_ref[2 * p + 1])).astype(BF16))
        ups = []
        for q in range(0, pairs, 2):
            x = jnp.concatenate([paired[q], paired[q + 1]], axis=1)
            ups.append(dot_t(x, diagonal(trans_ref[own[q]], trans_ref[own[q + 1]])).astype(BF16))
        for q, p in enumerate(own):
            coeff_ref[2 * p], coeff_ref[2 * p + 1] = dense(paired[q], mask)
        for q, up in enumerate(ups):
            p = own[2 * q]
            pay_ref[p], pay_ref[p + 1] = dense(up, mask)

    def edge(ref, first):
        lo = 0 if first else leaves - FAR
        for q in range(FAR):
            ref[q] = coeff_ref[lo + q]
        lo = 0 if first else leaves - NEAR
        for q in range(NEAR):
            x = pts_ref[lo + q]
            ref[FAR + 2 * q] = x[: n // 2]
            ref[FAR + 2 * q + 1] = x[n // 2 :]

    odd = me_ref[0] & 1 == 1

    @pl.when(odd)
    def _():
        edge(edge_ref, True)
        edge(side_ref, False)

    @pl.when(jnp.logical_not(odd))
    def _():
        edge(side_ref, True)
        edge(edge_ref, False)

    for c in listed:
        c.wait()
    place_ref[...] = (owner_ref[...] ^ me_ref[0]) * parents + local_ref[...]


def upward(me, points, basis, transfer, owner, local):
    leaves, n, _ = points.shape
    parents, rank, _ = transfer.shape
    steps = 2
    halo = FAR + 2 * NEAR
    tile = (n // 2, 2 * rank)
    smem = pl.BlockSpec(memory_space=pltpu.SMEM)
    vmem = pl.BlockSpec(memory_space=pltpu.VMEM)
    hbm = pl.BlockSpec(memory_space=pltpu.HBM)
    return pl.pallas_call(
        functools.partial(upward_kernel, steps=steps),
        out_shape=(
            jax.ShapeDtypeStruct((leaves,) + tile, BF16),
            jax.ShapeDtypeStruct((parents,) + tile, BF16),
            jax.ShapeDtypeStruct((halo,) + tile, BF16),
            jax.ShapeDtypeStruct((halo,) + tile, BF16),
            jax.ShapeDtypeStruct(owner.shape, jnp.int32),
        ),
        in_specs=[smem] + [hbm] * 5,
        out_specs=[vmem] * 5,
        scratch_shapes=[
            pltpu.VMEM(points.shape, BF16),
            pltpu.VMEM(basis.shape, BF16),
            pltpu.VMEM(transfer.shape, BF16),
            pltpu.VMEM(owner.shape, jnp.int32),
            pltpu.VMEM(owner.shape, jnp.int32),
            pltpu.SemaphoreType.DMA((3, steps)),
            pltpu.SemaphoreType.DMA((2,)),
        ],
        compiler_params=pltpu.CompilerParams(vmem_limit_bytes=LIMIT),
        name="upward",
    )(me, *[in_hbm(x) for x in (points, basis, transfer, owner, local)])


def local_kernel(
    me_ref, noff_hbm, coff_hbm, pts_hbm, near_hbm, coup_hbm, coeff_ref, *refs, leafs, base, stride, edges
):
    if edges:
        edge_ref, side_ref, hop_ref, *refs = refs
    near_out, field_out, noff_ref, coff_ref, pts_pad, coeff_pad, near_ref, coup_ref, sems, first_sems = refs
    leaves, n, _ = pts_hbm.shape
    steps, chunk, slots = near_ref.shape[:3]
    far_slots = coff_ref.shape[0]
    mask = left_half(n // 2, 128)

    def copies(i):
        own = pl.ds(base + stride * i, chunk)
        return (
            pltpu.make_async_copy(near_hbm.at[own], near_ref.at[i], sems.at[0, i]),
            pltpu.make_async_copy(coup_hbm.at[own], coup_ref.at[i], sems.at[1, i]),
        )

    early = (
        pltpu.make_async_copy(noff_hbm, noff_ref, first_sems.at[0]),
        pltpu.make_async_copy(coff_hbm, coff_ref, first_sems.at[1]),
        pltpu.make_async_copy(pts_hbm, pts_pad.at[pl.ds(NEAR, leaves)], first_sems.at[2]),
    )
    for c in early:
        c.start()
    for i in range(min(AHEAD, steps)):
        for c in copies(i):
            c.start()

    coeff_pad[FAR : FAR + leaves] = coeff_ref[...]

    def put(ref, low):
        co = 0 if low else leaves + FAR
        po = 0 if low else leaves + NEAR
        for q in range(FAR):
            coeff_pad[co + q] = ref[q]
        for q in range(NEAR):
            pts_pad[po + q, : n // 2] = ref[FAR + 2 * q]
            pts_pad[po + q, n // 2 :] = ref[FAR + 2 * q + 1]

    if edges:
        leaf = me_ref[0] & (leafs - 1)
        odd = leaf & 1 == 1

        def put_side(low):
            last = leaf == (0 if low else leafs - 1)

            @pl.when(last)
            def _():
                put(hop_ref, low)

            @pl.when(jnp.logical_not(last))
            def _():
                put(side_ref, low)

        @pl.when(odd)
        def _():
            put(edge_ref, True)
            put_side(False)

        @pl.when(jnp.logical_not(odd))
        def _():
            put_side(True)
            put(edge_ref, False)

    for c in early:
        c.wait()

    def body(i, carry):
        for c in copies(i):
            c.wait()

        @pl.when(i + AHEAD < steps)
        def _():
            for c in copies(i + AHEAD):
                c.start()

        nears, fields = [], []
        for j in range(chunk):
            c = base + stride * i + j
            xs = [pts_pad[c + NEAR + noff_ref[k, c]] for k in range(slots)]
            ws = [near_ref[i, j, k] for k in range(slots)]
            nears.append(dot_t(jnp.concatenate(xs, axis=1), jnp.concatenate(ws, axis=1)))
        for j in range(chunk):
            c = base + stride * i + j
            lhs = beside([coeff_pad[c + FAR + coff_ref[k, c]] for k in range(far_slots)], mask)
            fields.append(dot_t(lhs, coup_ref[i, j]))
        for j in range(chunk):
            near_out[i * chunk + j] = nears[j]
        for j in range(0, chunk, 2):
            field_out[(i * chunk + j) // 2] = jnp.concatenate([fields[j], fields[j + 1]], axis=1)
        return carry

    lax.fori_loop(0, steps, body, 0)


def local_terms(
    me, near_offsets, coupling_offsets, points, coeffs, halos, near_blocks, leaf_coupling, leafs, base, stride, steps, chunk
):
    leaves, n, size = points.shape
    rank = leaf_coupling.shape[1]
    tile = coeffs.shape[1:]
    smem = pl.BlockSpec(memory_space=pltpu.SMEM)
    vmem = pl.BlockSpec(memory_space=pltpu.VMEM)
    hbm = pl.BlockSpec(memory_space=pltpu.HBM)
    return pl.pallas_call(
        functools.partial(local_kernel, leafs=leafs, base=base, stride=stride, edges=bool(halos)),
        out_shape=(
            jax.ShapeDtypeStruct((steps * chunk, n, size), F32),
            jax.ShapeDtypeStruct((steps * chunk // 2, n, 2 * rank), F32),
        ),
        in_specs=[smem] + [hbm] * 5 + [vmem] * (1 + len(halos)),
        out_specs=[vmem] * 2,
        scratch_shapes=[
            pltpu.SMEM(near_offsets.shape, jnp.int32),
            pltpu.SMEM(coupling_offsets.shape, jnp.int32),
            pltpu.VMEM((leaves + 2 * NEAR, n, size), BF16),
            pltpu.VMEM((leaves + 2 * FAR,) + tile, BF16),
            pltpu.VMEM((steps, chunk) + near_blocks.shape[1:], BF16),
            pltpu.VMEM((steps, chunk) + leaf_coupling.shape[1:], BF16),
            pltpu.SemaphoreType.DMA((2, steps)),
            pltpu.SemaphoreType.DMA((3,)),
        ],
        compiler_params=pltpu.CompilerParams(vmem_limit_bytes=LIMIT),
        name="local_terms",
    )(
        me, *[in_hbm(x) for x in (near_offsets, coupling_offsets, points, near_blocks, leaf_coupling)],
        coeffs, *halos,
    )


def downward_kernel(
    place_hbm, table, coup_ref, trans_ref, basis_ref, near_mid, field_mid, near_rim, field_rim, out_hbm,
    place_ref, half_ref, total_ref, out_ref, sems, place_sem, *, batch
):
    parents = trans_ref.shape[0]
    n, size = near_mid.shape[1:]
    slots = place_ref.shape[0]
    mask = left_half(n // 2, 128)
    rim = field_rim.shape[0] // 2
    fetch = pltpu.make_async_copy(place_hbm, place_ref, place_sem)
    fetch.start()
    fetch.wait()

    def local_at(p):
        if rim <= p < parents - rim:
            return near_mid, field_mid, p - rim
        return near_rim, field_rim, p if p < rim else p - parents + 2 * rim

    def copy(step):
        own = pl.ds(2 * step * batch, 2 * batch)
        return pltpu.make_async_copy(out_ref.at[own], out_hbm.at[own], sems.at[step])

    for p in range(parents):
        tiles = [table[place_ref[k, p]] for k in range(slots)]
        half_ref[p] = dot_t(beside(tiles, mask), coup_ref[p]).astype(BF16)
    for p in range(parents):
        _, field_ref, at = local_at(p)
        total_ref[p] = (field_ref[at] + dot_n(half_ref[p], trans_ref[p])).astype(BF16)
    for step in range(parents // batch):
        for p in range(step * batch, (step + 1) * batch):
            near_ref, _, at = local_at(p)
            far = dot_n(total_ref[p], diagonal(basis_ref[2 * p], basis_ref[2 * p + 1]))
            out_ref[2 * p] = (far[:, :size] + near_ref[2 * at]).astype(BF16)
            out_ref[2 * p + 1] = (far[:, size:] + near_ref[2 * at + 1]).astype(BF16)
        copy(step).start()
    for step in range(parents // batch):
        copy(step).wait()


def downward(place, table, coupling, transfer, basis, mid, rim):
    leaves, _, size = basis.shape
    n = mid[0].shape[1]
    vmem = pl.BlockSpec(memory_space=pltpu.VMEM)
    big = [pltpu.with_memory_space_constraint(x, pltpu.VMEM) for x in (table, coupling, transfer, basis, *mid, *rim)]
    parents, rank, _ = transfer.shape
    batch = parents // 4
    return pl.pallas_call(
        functools.partial(downward_kernel, batch=batch),
        out_shape=jax.ShapeDtypeStruct((leaves, n, size), BF16),
        in_specs=[pl.BlockSpec(memory_space=pl.ANY)] + [vmem] * len(big),
        out_specs=pl.BlockSpec(memory_space=pltpu.HBM),
        scratch_shapes=[
            pltpu.SMEM(place.shape, jnp.int32),
            pltpu.VMEM((parents, n, rank), BF16),
            pltpu.VMEM((parents, n, 2 * rank), BF16),
            pltpu.VMEM((leaves, n, size), BF16),
            pltpu.SemaphoreType.DMA((parents // batch,)),
            pltpu.SemaphoreType.DMA,
        ],
        compiler_params=pltpu.CompilerParams(vmem_limit_bytes=LIMIT),
        name="downward",
    )(place, *big)


def on_device(
    points_rhs,
    leaf_basis,
    transfer,
    leaf_coupling,
    parent_coupling,
    near_blocks,
    near_offsets,
    coupling_offsets,
    parent_owner,
    parent_local,
):
    streams, leafs = lax.axis_size("stream"), lax.axis_size("leaf")
    devices = streams * leafs
    me = lax.axis_index(AXES).astype(jnp.int32)
    flag = me.reshape(1)

    my_leaf = me % leafs

    def permute(x, pairs):
        return lax.ppermute(x, AXES, pairs)

    def swap(x, bits):
        return permute(x, [(i, i ^ bits) for i in range(devices)])

    coeffs, own, edge, side, place = upward(flag, points_rhs, leaf_basis, transfer, parent_owner.T, parent_local.T)

    line = [own] + [swap(own, k) for k in range(1, leafs)]
    edges = swap(edge, 1)
    sides, k = None, 3
    while k < leafs:
        both = swap(side, k)
        if sides is None:
            sides = both
        else:
            away = my_leaf ^ jnp.where(my_leaf % 2 == 1, my_leaf + 1, my_leaf - 1)
            sides = jnp.where((away == k) | (k == leafs - 1) & (away > k) | (away < 0), both, sides)
        k = 2 * k + 1
    ends = [(s * leafs, (s + 1) * leafs) for s in range(streams - 1)]
    ends += [(s * leafs + leafs - 1, s * leafs - 1) for s in range(1, streams)]
    hop = permute(sides, ends)

    def join(parts):
        return parts[0] if len(parts) == 1 else jnp.concatenate(parts, axis=0)

    groups = [(0, [join(line[:2])]), (2, [join(line[2:])])]
    pieces = {}
    for base, parts in groups:
        have = {0: parts}
        for s in range(2, streams, 2):
            low = s & -s
            high = 1 << (s.bit_length() - 1)
            if low == high:
                have[s] = [swap(x, s * leafs) for x in have[s ^ low]]
                continue
            near, far = have[s ^ low], have[s ^ high]
            if len(near) == 1:
                rows = near[0].shape[0] // 2
                near, far = (near[0][:rows], None), (None, far[0][rows:])
            have[s] = [swap(far[j], high * leafs) if j % 2 else swap(near[j], low * leafs) for j in range(len(near))]
        for s in list(have):
            have[s] = join(have[s])
            have[s ^ 1] = swap(have[s], leafs)
        for s, g in have.items():
            pieces[s * leafs + base] = g
    table = jnp.concatenate([pieces[k] for k in sorted(pieces)], axis=0)

    leaves = points_rhs.shape[0]
    rim = 8
    chunk = (leaves - 2 * rim) // 6
    args = (flag, near_offsets.T, coupling_offsets.T, points_rhs, coeffs)
    mid = local_terms(*args, (), near_blocks, leaf_coupling, leafs, rim, chunk, 6, chunk)
    edge = local_terms(*args, (edges, sides, hop), near_blocks, leaf_coupling, leafs, 0, leaves - rim, 2, rim)
    return downward(place, table, parent_coupling, transfer, leaf_basis, mid, edge)


def solution(mesh):
    three = P(AXES, None, None)
    two = P(AXES, None)
    return jax.shard_map(
        on_device,
        mesh=mesh,
        in_specs=(three,) * 5 + (P(AXES, None, None, None),) + (two,) * 4,
        out_specs=three,
        check_vma=False,
    )
```
